8 devices in a mesh: replica: 2 (over z, y), model: 4 (over x, core).
Axes of the slice: x: 2, y: 2, z: 1, core: 2. Of those that a mesh axis runs over, the one named last changes fastest.
Arguments:
- tokens: bfloat16 [256, 3072], P('replica'), parts along dimension 0
- lengths: int32 [256], P('replica'), parts along dimension 0
- k_cache: bfloat16 [256, 8, 512, 128], P('replica'), parts along dimension 0
- v_cache: bfloat16 [256, 8, 512, 128], P('replica'), parts along dimension 0
- norm_gain: bfloat16 [3072], replicated
- w_query: bfloat16 [3072, 3072], P(None, 'model')
- w_key: bfloat16 [3072, 1024], replicated
- w_value: bfloat16 [3072, 1024], replicated
- w_out: bfloat16 [3072, 3072], P('model')
- w_gate: bfloat16 [3072, 12288], P(None, 'model')
- w_up: bfloat16 [3072, 12288], P(None, 'model')
- w_down: bfloat16 [12288, 3072], P('model')
Outputs:
- output 1: bfloat16 [256, 3072], P('replica'), parts along dimension 0
- output 2: bfloat16 [256, 8, 128], P(('replica', 'model')), parts along dimension 0
- output 3: bfloat16 [256, 8, 128], P(('replica', 'model')), parts along dimension 0
There are 2 independent parts. The reference program is written for one: setup_inputs(seed, part) draws one part's arguments, and reference() takes and returns one part's arrays. A program takes and returns all parts, laid end to end along the dimension named above; an argument that names none is the same for every part.
All inputs are finite; a program needn't handle non-finite values.
Results may differ from the reference program's by a relative error of at most 0.00484794.
Values are sent between devices in bfloat16 or wider.
A program may use at most 1.5 GiB of HBM per device.

```python
import math
import jax
import jax.numpy as jnp
from jax import lax

MODEL_DIM = 3072
HEADS = 24
KV_HEADS = 8
HEAD_DIM = 128
FFN_DIM = 12288
BATCH_SIZE = 128
CONTEXT = 512

ROPE_BASE = 10000.0
NORM_EPS = 1e-6
MASK_VALUE = -1e30
KEY_SCALE = math.sqrt(math.log(CONTEXT))
LOG_CONTEXT = int(math.log2(CONTEXT))


def normal_weight(rng_key, fan_in, fan_out, gain):
    return jax.random.normal(rng_key, (fan_in, fan_out), jnp.float32) * (gain / math.sqrt(fan_in))


def setup_inputs(seed: int = 0, part: int = 0) -> dict:
    part_keys = jax.random.split(jax.random.fold_in(jax.random.key(seed), part), 8)
    shared_keys = jax.random.split(jax.random.key(seed + 1), 8)
    query_width = HEADS * HEAD_DIM
    kv_width = KV_HEADS * HEAD_DIM
    tokens = jax.random.normal(part_keys[0], (BATCH_SIZE, MODEL_DIM), jnp.float32)
    spans = jax.random.randint(part_keys[1], (BATCH_SIZE,), 0, CONTEXT - 1)
    shifts = jax.random.randint(part_keys[2], (BATCH_SIZE,), 0, LOG_CONTEXT + 1)
    lengths = 1 + jnp.right_shift(spans, shifts)
    row_ids = jnp.arange(BATCH_SIZE)
    long_row = jax.random.randint(part_keys[3], (), 0, BATCH_SIZE)
    short_row = (long_row + jax.random.randint(part_keys[4], (), 1, BATCH_SIZE)) % BATCH_SIZE
    lengths = jnp.where(row_ids == long_row, CONTEXT - 1, lengths)
    lengths = jnp.where(row_ids == short_row, 1, lengths).astype(jnp.int32)
    cache_shape = (BATCH_SIZE, KV_HEADS, CONTEXT, HEAD_DIM)
    k_cache = jax.random.normal(part_keys[5], cache_shape, jnp.float32) * KEY_SCALE
    v_cache = jax.random.normal(part_keys[6], cache_shape, jnp.float32)
    norm_gain = jax.random.uniform(shared_keys[0], (MODEL_DIM,), jnp.float32, 0.5, 1.5)
    w_query = normal_weight(shared_keys[1], MODEL_DIM, query_width, 1.0)
    w_key = normal_weight(shared_keys[2], MODEL_DIM, kv_width, KEY_SCALE)
    w_value = normal_weight(shared_keys[3], MODEL_DIM, kv_width, 1.0)
    w_out = normal_weight(shared_keys[4], query_width, MODEL_DIM, 1.0)
    w_gate = normal_weight(shared_keys[5], MODEL_DIM, FFN_DIM, 1.0)
    w_up = normal_weight(shared_keys[6], MODEL_DIM, FFN_DIM, 1.0)
    w_down = normal_weight(shared_keys[7], FFN_DIM, MODEL_DIM, 1.0)
    return {
        'tokens': tokens.astype(jnp.bfloat16),
        'lengths': lengths,
        'k_cache': k_cache.astype(jnp.bfloat16),
        'v_cache': v_cache.astype(jnp.bfloat16),
        'norm_gain': norm_gain.astype(jnp.bfloat16),
        'w_query': w_query.astype(jnp.bfloat16),
        'w_key': w_key.astype(jnp.bfloat16),
        'w_value': w_value.astype(jnp.bfloat16),
        'w_out': w_out.astype(jnp.bfloat16),
        'w_gate': w_gate.astype(jnp.bfloat16),
        'w_up': w_up.astype(jnp.bfloat16),
        'w_down': w_down.astype(jnp.bfloat16),
    }


def rms_norm(tokens, norm_gain):
    values = tokens.astype(jnp.float32)
    mean_sq = jnp.mean(values * values, axis=-1, keepdims=True)
    return (values * lax.rsqrt(mean_sq + NORM_EPS) * norm_gain.astype(jnp.float32)).astype(jnp.bfloat16)


def apply_rope(values, positions):
    half_dim = values.shape[-1] // 2
    inv_freq = jnp.exp(jnp.arange(half_dim, dtype=jnp.float32) * (-2.0 * math.log(ROPE_BASE) / values.shape[-1]))
    angles = positions.astype(jnp.float32)[:, None, None] * inv_freq[None, None, :]
    cos_part = jnp.cos(angles)
    sin_part = jnp.sin(angles)
    first_half = values[..., :half_dim]
    second_half = values[..., half_dim:]
    return jnp.concatenate([first_half * cos_part - second_half * sin_part, second_half * cos_part + first_half * sin_part], axis=-1)


def reference(tokens, lengths, k_cache, v_cache, norm_gain, w_query, w_key, w_value, w_out, w_gate, w_up, w_down):
    group_size = HEADS // KV_HEADS
    scale = HEAD_DIM ** -0.5
    normed = rms_norm(tokens, norm_gain)
    queries = apply_rope(jnp.dot(normed, w_query, preferred_element_type=jnp.float32).reshape(BATCH_SIZE, HEADS, HEAD_DIM), lengths).astype(jnp.bfloat16)
    new_keys = apply_rope(jnp.dot(normed, w_key, preferred_element_type=jnp.float32).reshape(BATCH_SIZE, KV_HEADS, HEAD_DIM), lengths).astype(jnp.bfloat16)
    new_values = jnp.dot(normed, w_value, preferred_element_type=jnp.float32).reshape(BATCH_SIZE, KV_HEADS, HEAD_DIM).astype(jnp.bfloat16)
    positions = jnp.arange(CONTEXT)

    def one_sequence(items):
        query_row, key_rows, value_rows, key_new, value_new, length = items
        grouped = query_row.reshape(KV_HEADS, group_size, HEAD_DIM).astype(jnp.float32)
        scores = jnp.einsum('grd,gtd->grt', grouped, key_rows.astype(jnp.float32)) * scale
        scores = jnp.where(positions[None, None, :] < length, scores, MASK_VALUE)
        score_new = jnp.einsum('grd,gd->gr', grouped, key_new.astype(jnp.float32)) * scale
        peak = jnp.maximum(jnp.max(scores, axis=-1), score_new)
        weights = jnp.exp(scores - peak[:, :, None])
        weight_new = jnp.exp(score_new - peak)
        total = jnp.sum(weights, axis=-1) + weight_new
        mixed = jnp.einsum('grt,gtd->grd', weights.astype(jnp.bfloat16).astype(jnp.float32), value_rows.astype(jnp.float32))
        mixed = mixed + weight_new.astype(jnp.bfloat16).astype(jnp.float32)[:, :, None] * value_new.astype(jnp.float32)[:, None, :]
        return (mixed / total[:, :, None]).astype(jnp.bfloat16).reshape(HEADS * HEAD_DIM)

    attended = lax.map(one_sequence, (queries, k_cache, v_cache, new_keys, new_values, lengths))
    gate_act = jnp.dot(normed, w_gate, preferred_element_type=jnp.float32)
    up_act = jnp.dot(normed, w_up, preferred_element_type=jnp.float32)
    hidden = (jax.nn.silu(gate_act) * up_act).astype(jnp.bfloat16)
    summed = tokens.astype(jnp.float32) + jnp.dot(attended, w_out, preferred_element_type=jnp.float32) + jnp.dot(hidden, w_down, preferred_element_type=jnp.float32)
    return summed.astype(jnp.bfloat16), new_keys, new_values
```

```python
import functools
import math

import jax
import jax.numpy as jnp
from jax import lax
from jax.experimental import pallas as pl
from jax.experimental.pallas import tpu as pltpu
from jax.sharding import PartitionSpec as P

ROPE_BASE = 10000.0
NORM_EPS = 1e-6
MASK_VALUE = -1e30
MESH = pl.DeviceIdType.MESH
F32 = jnp.float32
BF16 = jnp.bfloat16
TILE = 256
SLOTS = 8
AHEAD = SLOTS // 2


def rms_norm(tokens, norm_gain):
    values = tokens.astype(F32)
    mean_sq = jnp.mean(values * values, axis=-1, keepdims=True)
    return (values * lax.rsqrt(mean_sq + NORM_EPS) * norm_gain.astype(F32)).astype(BF16)


def apply_rope(values, positions):
    half_dim = values.shape[-1] // 2
    inv_freq = jnp.exp(jnp.arange(half_dim, dtype=F32) * (-2.0 * math.log(ROPE_BASE) / values.shape[-1]))
    angles = positions.astype(F32)[:, None, None] * inv_freq[None, None, :]
    cos_part = jnp.cos(angles)
    sin_part = jnp.sin(angles)
    first_half = values[..., :half_dim]
    second_half = values[..., half_dim:]
    return jnp.concatenate([first_half * cos_part - second_half * sin_part, second_half * cos_part + first_half * sin_part], axis=-1)


def attend(queries, key_rows, value_rows, key_new, value_new, row_lengths):
    row_count, heads, head_dim = queries.shape
    kv_heads = key_rows.shape[1]
    grouped = queries.reshape(row_count, kv_heads, heads // kv_heads, head_dim)
    scale = head_dim ** -0.5
    scores = jnp.einsum('bgrd,bgtd->bgrt', grouped, key_rows, preferred_element_type=F32) * scale
    valid = jnp.arange(key_rows.shape[2])[None, None, None, :] < row_lengths[:, None, None, None]
    scores = jnp.where(valid, scores, MASK_VALUE)
    score_new = jnp.einsum('bgrd,bgd->bgr', grouped, key_new, preferred_element_type=F32) * scale
    peak = jnp.maximum(jnp.max(scores, axis=-1), score_new)
    weights = jnp.exp(scores - peak[..., None])
    weight_new = jnp.exp(score_new - peak)
    total = jnp.sum(weights, axis=-1) + weight_new
    mixed = jnp.einsum('bgrt,bgtd->bgrd', weights.astype(BF16), value_rows, preferred_element_type=F32)
    mixed = mixed + weight_new.astype(BF16).astype(F32)[..., None] * value_new.astype(F32)[:, :, None, :]
    return (mixed / total[..., None]).astype(BF16).reshape(row_count, heads * head_dim)


def mlp_kernel(normed, tokens, attended, kv_new, w_gate, w_up, w_down, w_out,
               y_out, key_out, value_out,
               h_buf, x_buf, o_buf, kv_buf, w_buf, wo_buf, u_buf, part, from_sib, to_cross, from_cross, y_buf, kv_in, head_buf,
               in_sem, w_sem, wo_sem, kv_send, kv_recv, s1_send, s1_recv, s2_send, s2_recv,
               yc_send, yc_recv, ys_send, ys_recv, yr_send, yr_recv, out_sem):
    me = lax.axis_index('model')
    core = lax.rem(me, 2)
    chip = lax.div(me, 2)
    sib = chip * 2 + (1 - core)
    cross = (1 - chip) * 2 + core
    diag = (1 - chip) * 2 + (1 - core)
    model_dim = w_gate.shape[0]
    width = w_gate.shape[1]
    n_hid = width // TILE
    n_out = model_dim // TILE
    head_dim = head_buf.shape[2]
    local_kv = kv_new.shape[2] // (2 * head_dim)

    barrier = pltpu.get_barrier_semaphore()
    for peer in (sib, cross, diag):
        pl.semaphore_signal(barrier, inc=1, device_id={'model': peer}, device_id_type=MESH)

    def cols(tile):
        return pl.ds(pl.multiple_of(tile * TILE, TILE), TILE)

    def fetch(src, tile, slot):
        return pltpu.make_async_copy(src.at[:, cols(tile)], w_buf.at[slot], w_sem.at[slot])

    def remote(src, dst, send, recv, peer):
        return pltpu.make_async_remote_copy(src_ref=src, dst_ref=dst, send_sem=send, recv_sem=recv,
                                            device_id={'model': peer}, device_id_type=MESH)

    h_copy = pltpu.make_async_copy(normed, h_buf, in_sem.at[0])
    h_copy.start()
    for pair in range(AHEAD):
        fetch(w_gate, pair, 2 * pair).start()
        fetch(w_up, pair, 2 * pair + 1).start()
    x_copy = pltpu.make_async_copy(tokens.at[me], x_buf, in_sem.at[1])
    o_copy = pltpu.make_async_copy(attended, o_buf, in_sem.at[2])
    kv_copy = pltpu.make_async_copy(kv_new, kv_buf, in_sem.at[3])
    for copy in (x_copy, o_copy, kv_copy):
        copy.start()
    h_copy.wait()

    def hidden_tile(j):
        slot = lax.rem(2 * j, SLOTS)
        fetch(w_gate, j, slot).wait()
        gate = jnp.dot(h_buf[...], w_buf[slot], preferred_element_type=F32)
        fetch(w_up, j, slot + 1).wait()
        up = jnp.dot(h_buf[...], w_buf[slot + 1], preferred_element_type=F32)
        u_buf[:, cols(j)] = (jax.nn.silu(gate) * up).astype(BF16)
        return slot

    @pl.loop(0, n_hid - AHEAD)
    def _(j):
        slot = hidden_tile(j)
        fetch(w_gate, j + AHEAD, slot).start()
        fetch(w_up, j + AHEAD, slot + 1).start()

    wo_copy = pltpu.make_async_copy(w_out, wo_buf, wo_sem)
    wo_copy.start()
    kv_copy.wait()
    pl.semaphore_wait(barrier, 3)
    kv_sends = []
    for n, peer in enumerate((sib, cross, diag)):
        send = remote(kv_buf.at[peer], kv_in.at[me], kv_send.at[n], kv_recv.at[n], peer)
        send.start()
        kv_sends.append(send)

    @pl.loop(n_hid - AHEAD, n_hid)
    def _(j):
        slot = hidden_tile(j)
        tile = 2 * (j - (n_hid - AHEAD))
        fetch(w_down, tile, slot).start()
        fetch(w_down, tile + 1, slot + 1).start()

    x_copy.wait()
    o_copy.wait()
    wo_copy.wait()

    def sib_send(c):
        return remote(part.at[c, :, 1 - core], from_sib.at[c], s1_send.at[c], s1_recv.at[c], sib)

    def cross_send(c):
        return remote(to_cross.at[c], from_cross.at[c], s2_send.at[c], s2_recv.at[c], cross)

    def y_cross(c):
        return remote(y_buf.at[c, me], y_buf.at[c, me], yc_send.at[c], yc_recv.at[c], cross)

    def y_sib(c):
        return remote(y_buf.at[c, me], y_buf.at[c, me], ys_send.at[c], ys_recv.at[c], sib)

    def y_relay(c):
        return remote(y_buf.at[c, cross], y_buf.at[c, cross], yr_send.at[c], yr_recv.at[c], sib)

    def y_store(c):
        return pltpu.make_async_copy(y_buf.at[c], y_out.at[:, :, cols(c)], out_sem.at[c])

    @pl.loop(0, n_out + 6)
    def _(i):
        @pl.when(i < n_out)
        def _():
            slot = lax.rem(i, SLOTS)
            fetch(w_down, i, slot).wait()
            total = jnp.dot(u_buf[...], w_buf[slot], preferred_element_type=F32)
            total += jnp.dot(o_buf[...], wo_buf[:, cols(i)], preferred_element_type=F32)
            part[i] = total.reshape(part.shape[1:])
            sib_send(i).start()

        @pl.when(i < n_out - SLOTS)
        def _():
            fetch(w_down, i + SLOTS, lax.rem(i, SLOTS)).start()

        @pl.when((i >= 1) & (i < n_out + 1))
        def _():
            c = i - 1
            sib_send(c).wait_recv()
            to_cross[c] = part[c, 1 - chip, core] + from_sib[c, 1 - chip]
            cross_send(c).start()

        @pl.when((i >= 3) & (i < n_out + 3))
        def _():
            c = i - 3
            cross_send(c).wait_recv()
            total = part[c, chip, core] + from_sib[c, chip] + from_cross[c]
            y_buf[c, me] = (x_buf[:, cols(c)].astype(F32) + total).astype(BF16)
            y_cross(c).start()
            y_sib(c).start()

        @pl.when((i >= 5) & (i < n_out + 5))
        def _():
            c = i - 5
            y_cross(c).wait_recv()
            y_relay(c).start()

        @pl.when(i == n_out)
        def _():
            for send in kv_sends:
                send.wait_recv()
            kv_in[me] = kv_buf[me]
            for half, out in enumerate((key_out, value_out)):
                for source in range(kv_in.shape[0]):
                    for g in range(local_kv):
                        start = (half * local_kv + g) * head_dim
                        head_buf[:, source * local_kv + g, :] = kv_in[source, :, start:start + head_dim].astype(F32)
                out[...] = head_buf[...].astype(BF16)

        @pl.when(i >= 6)
        def _():
            c = i - 6
            y_sib(c).wait_recv()
            y_relay(c).wait_recv()
            y_store(c).start()

    for send in kv_sends:
        send.wait_send()

    @pl.loop(0, n_out)
    def _(c):
        sib_send(c).wait_send()
        cross_send(c).wait_send()
        y_cross(c).wait_send()
        y_sib(c).wait_send()
        y_relay(c).wait_send()
        y_store(c).wait()


def mlp_and_sum(normed, tokens, attended, kv_new, w_gate, w_up, w_down, w_out, kv_heads, head_dim):
    batch, model_dim = normed.shape
    width = w_gate.shape[1]
    q_dim = w_out.shape[0]
    devices = 4
    rows = batch // devices
    n_out = model_dim // TILE
    kv_width = kv_new.shape[1]
    dma = pltpu.SemaphoreType.DMA
    hbm = pl.BlockSpec(memory_space=pl.ANY)
    vmem = pl.BlockSpec(memory_space=pltpu.VMEM)
    y, key_out, value_out = pl.pallas_call(
        mlp_kernel,
        out_shape=(jax.ShapeDtypeStruct((devices, rows, model_dim), BF16),
                   jax.ShapeDtypeStruct((rows, kv_heads, head_dim), BF16),
                   jax.ShapeDtypeStruct((rows, kv_heads, head_dim), BF16)),
        in_specs=[hbm] * 8,
        out_specs=(hbm, vmem, vmem),
        scratch_shapes=[
            pltpu.VMEM((batch, model_dim), BF16),
            pltpu.VMEM((rows, model_dim), BF16),
            pltpu.VMEM((batch, q_dim), BF16),
            pltpu.VMEM((devices, rows, kv_width), BF16),
            pltpu.VMEM((SLOTS, model_dim, TILE), BF16),
            pltpu.VMEM((q_dim, model_dim), BF16),
            pltpu.VMEM((batch, width), BF16),
            pltpu.VMEM((n_out, 2, 2, rows, TILE), F32),
            pltpu.VMEM((n_out, 2, rows, TILE), F32),
            pltpu.VMEM((n_out, rows, TILE), F32),
            pltpu.VMEM((n_out, rows, TILE), F32),
            pltpu.VMEM((n_out, devices, rows, TILE), BF16),
            pltpu.VMEM((devices, rows, kv_width), BF16),
            pltpu.VMEM((rows, kv_heads, head_dim), F32),
            dma((4,)), dma((SLOTS,)), dma, dma((3,)), dma((3,)),
        ] + [dma((n_out,))] * 11,
        compiler_params=pltpu.CompilerParams(collective_id=0, has_side_effects=True, vmem_limit_bytes=48 * 2 ** 20),
        name="mlp_and_sum",
    )(normed, tokens.reshape(devices, rows, model_dim), attended, kv_new.reshape(devices, rows, kv_width), w_gate, w_up, w_down, w_out)
    return y.reshape(batch, model_dim), key_out, value_out


def solution(mesh):
    groups = mesh.shape['model']

    def local_step(tokens, lengths, k_cache, v_cache, norm_gain, w_query, w_key, w_value, w_out, w_gate, w_up, w_down):
        batch = tokens.shape[0]
        kv_heads = k_cache.shape[1]
        head_dim = k_cache.shape[3]
        local_heads = w_query.shape[1] // head_dim
        local_kv = kv_heads // groups
        me = lax.axis_index('model')
        normed = rms_norm(tokens, norm_gain)
        queries = apply_rope(jnp.dot(normed, w_query, preferred_element_type=F32).reshape(batch, local_heads, head_dim), lengths).astype(BF16)
        wk = lax.dynamic_slice_in_dim(w_key, me * local_kv * head_dim, local_kv * head_dim, 1)
        wv = lax.dynamic_slice_in_dim(w_value, me * local_kv * head_dim, local_kv * head_dim, 1)
        key_new = apply_rope(jnp.dot(normed, wk, preferred_element_type=F32).reshape(batch, local_kv, head_dim), lengths).astype(BF16)
        value_new = jnp.dot(normed, wv, preferred_element_type=F32).reshape(batch, local_kv, head_dim).astype(BF16)
        key_rows = lax.dynamic_slice_in_dim(k_cache, me * local_kv, local_kv, 1)
        value_rows = lax.dynamic_slice_in_dim(v_cache, me * local_kv, local_kv, 1)
        attended = attend(queries, key_rows, value_rows, key_new, value_new, lengths)
        kv_new = jnp.concatenate([key_new.reshape(batch, -1), value_new.reshape(batch, -1)], axis=1)
        return mlp_and_sum(normed, tokens, attended, kv_new, w_gate, w_up, w_down, w_out, kv_heads, head_dim)

    in_specs = (P('replica', None), P('replica'), P('replica', None, None, None), P('replica', None, None, None), P(None), P(None, 'model'), P(None, None), P(None, None), P('model', None), P(None, 'model'), P(None, 'model'), P('model', None))
    out_specs = (P('replica', None), P(('replica', 'model'), None, None), P(('replica', 'model'), None, None))
    return jax.shard_map(local_step, mesh=mesh, in_specs=in_specs, out_specs=out_specs, check_vma=False)
```

```python
import functools
import math

import jax
import jax.numpy as jnp
from jax import lax
from jax.experimental import pallas as pl
from jax.experimental.pallas import tpu as pltpu
from jax.sharding import PartitionSpec as P

ROPE_BASE = 10000.0
NORM_EPS = 1e-6
MASK_VALUE = -1e30
MESH = pl.DeviceIdType.MESH
F32 = jnp.float32
BF16 = jnp.bfloat16
TILE = 256
SLOTS = 8
AHEAD = SLOTS // 2


CHUNK = 64
GROUP = 32
UNROLL = 8


def rope_tables(positions, head_dim):
    half_dim = head_dim // 2
    inv_freq = jnp.exp(jnp.arange(half_dim, dtype=F32) * (-2.0 * math.log(ROPE_BASE) / head_dim))
    angles = positions.astype(F32)[:, None] * inv_freq[None, :]
    cos_part = jnp.cos(angles)
    sin_part = jnp.sin(angles)
    return jnp.concatenate([cos_part, cos_part], axis=-1), jnp.concatenate([-sin_part, sin_part], axis=-1)


def attend_kernel(lengths, tokens, gain, cos_part, sin_part, k_cache, v_cache, w_query, w_key, w_value,
                  h_out, o_out, kv_out,
                  x_buf, w_buf, k_buf, v_buf, q_buf, kn_buf, vn_buf, score, peak, total, mixed,
                  item_row, item_pos, count, x_sem, w_sem, k_sem, v_sem):
    batch, model_dim = tokens.shape
    head_dim = cos_part.shape[1]
    local_kv = kv_out.shape[1] // (2 * head_dim)
    heads = o_out.shape[1] // head_dim
    ratio = heads // local_kv
    q_tiles = w_query.shape[1] // TILE
    per_tile = TILE // head_dim
    n_groups = batch // GROUP
    scale = head_dim ** -0.5
    me = lax.axis_index('model')
    first_kv = me * local_kv

    x_copy = pltpu.make_async_copy(tokens, x_buf, x_sem)
    x_copy.start()
    kv_cols = pl.ds(pl.multiple_of(me * TILE, TILE), TILE)
    w_copies = [pltpu.make_async_copy(w_query.at[:, t * TILE:(t + 1) * TILE], w_buf.at[t], w_sem.at[t]) for t in range(q_tiles)]
    w_copies.append(pltpu.make_async_copy(w_key.at[:, kv_cols], w_buf.at[q_tiles], w_sem.at[q_tiles]))
    w_copies.append(pltpu.make_async_copy(w_value.at[:, kv_cols], w_buf.at[q_tiles + 1], w_sem.at[q_tiles + 1]))
    for copy in w_copies:
        copy.start()

    def fetch(cache, buf, sem, seq, row, pos, par):
        return pltpu.make_async_copy(cache.at[seq, pl.ds(first_kv, local_kv), pl.ds(pl.multiple_of(pos, CHUNK), CHUNK)],
                                     buf.at[par, row, :, pl.ds(pl.multiple_of(pos, CHUNK), CHUNK)], sem.at[par])

    def issue(g):
        par = g % 2

        def one_seq(row, k):
            seq = g * GROUP + row

            def one_chunk(c, k):
                pos = c * CHUNK
                fetch(k_cache, k_buf, k_sem, seq, row, pos, par).start()
                fetch(v_cache, v_buf, v_sem, seq, row, pos, par).start()
                item_row[par, k] = row
                item_pos[par, k] = pos
                return k + 1

            return lax.fori_loop(0, lax.div(lengths[seq] + (CHUNK - 1), CHUNK), one_chunk, k)

        n = lax.fori_loop(0, GROUP, one_seq, 0)
        for u in range(UNROLL - 1):
            item_row[par, n + u] = GROUP
            item_pos[par, n + u] = 0
        count[par] = n

    issue(0)
    issue(1)

    x_copy.wait()
    x = x_buf[...].astype(F32)
    mean_sq = jnp.mean(x * x, axis=-1, keepdims=True)
    h_out[...] = (x * lax.rsqrt(mean_sq + NORM_EPS) * gain[...].astype(F32)).astype(BF16)

    def rope(a):
        return a * cos_part[...] + pltpu.roll(a, head_dim // 2, 1) * sin_part[...]

    for t, copy in enumerate(w_copies):
        copy.wait()
        prod = jnp.dot(h_out[...], w_buf[t], preferred_element_type=F32)
        for j in range(per_tile):
            a = prod[:, j * head_dim:(j + 1) * head_dim]
            if t < q_tiles:
                q_buf[:, t * per_tile + j, :] = rope(a).astype(BF16).astype(F32)
            else:
                a = (rope(a) if t == q_tiles else a).astype(BF16)
                col = ((t - q_tiles) * local_kv + j) * head_dim
                kv_out[:, col:col + head_dim] = a
                for r in range(ratio):
                    (kn_buf if t == q_tiles else vn_buf)[:, j * ratio + r, :] = a.astype(F32)
    for h in range(heads, q_buf.shape[1]):
        zero = jnp.zeros((batch, head_dim), F32)
        q_buf[:, h, :] = zero
        kn_buf[:, h, :] = zero
        vn_buf[:, h, :] = zero

    sub = q_buf.shape[1]
    lane = lax.broadcasted_iota(jnp.int32, (sub, local_kv * CHUNK), 1)
    head = lax.broadcasted_iota(jnp.int32, (sub, local_kv * CHUNK), 0)
    own = (lax.div(lane, CHUNK) == lax.div(head, ratio)) & (head < heads)
    pos_in = jnp.where(own, lax.rem(lane, CHUNK), 1 << 20)

    for g in range(n_groups):
        par = g % 2
        base = g * GROUP
        n = count[par]
        steps = lax.div(n + (UNROLL - 1), UNROLL)

        def wait_all(cache, buf, sem):
            @pl.loop(0, n)
            def _(k):
                fetch(cache, buf, sem, 0, 0, 0, par).wait()

        peak[...] = jnp.full(peak.shape, MASK_VALUE, F32)
        total[...] = jnp.zeros(total.shape, F32)
        mixed[...] = jnp.zeros(mixed.shape, F32)
        wait_all(k_cache, k_buf, k_sem)

        def slot(k):
            row = item_row[par, k]
            pos = item_pos[par, k]
            return row, jnp.minimum(row, GROUP - 1), pos

        @pl.loop(0, steps)
        def _(step):
            found = []
            for u in range(UNROLL):
                k = step * UNROLL + u
                row, at, pos = slot(k)
                keys = k_buf[par, at, :, pl.ds(pl.multiple_of(pos, CHUNK), CHUNK), :].reshape(local_kv * CHUNK, head_dim)
                s = lax.dot_general(q_buf[base + at].astype(BF16), keys, (((1,), (1,)), ((), ())), preferred_element_type=F32) * scale
                s = jnp.where(pos_in < jnp.where(row < GROUP, lengths[base + at], 0) - pos, s, MASK_VALUE)
                score[k] = s
                found.append((row, s))
            for row, s in found:
                peak[row] = jnp.maximum(peak[row], s)

        q = q_buf[base:base + GROUP]
        score_new = jnp.sum(q * kn_buf[base:base + GROUP], axis=-1, keepdims=True) * scale
        top = jnp.maximum(jnp.max(peak[:GROUP], axis=-1, keepdims=True), score_new)
        weight_new = jnp.exp(score_new - top)
        peak[:GROUP] = jnp.broadcast_to(top, (GROUP, sub, peak.shape[2]))

        wait_all(v_cache, v_buf, v_sem)

        @pl.loop(0, steps)
        def _(step):
            found = []
            for u in range(UNROLL):
                k = step * UNROLL + u
                row, at, pos = slot(k)
                p = jnp.exp(score[k] - peak[at])
                values = v_buf[par, at, :, pl.ds(pl.multiple_of(pos, CHUNK), CHUNK), :].reshape(local_kv * CHUNK, head_dim)
                found.append((row, p, jnp.dot(p.astype(BF16), values, preferred_element_type=F32)))
            for row, p, o in found:
                total[row] = total[row] + p
                mixed[row] = mixed[row] + o

        if g + 2 < n_groups:
            issue(g + 2)
        norm = jnp.sum(total[:GROUP], axis=-1, keepdims=True) + weight_new
        out = mixed[:GROUP] + weight_new.astype(BF16).astype(F32) * vn_buf[base:base + GROUP]
        q_buf[base:base + GROUP] = out / norm

    for h in range(heads):
        o_out[:, h * head_dim:(h + 1) * head_dim] = q_buf[:, h, :].astype(BF16)


def qkv_and_attend(tokens, lengths, k_cache, v_cache, norm_gain, w_query, w_key, w_value, groups):
    batch, model_dim = tokens.shape
    kv_heads, context, head_dim = k_cache.shape[1:]
    local_kv = kv_heads // groups
    q_dim = w_query.shape[1]
    cos_part, sin_part = rope_tables(lengths, head_dim)
    items = GROUP * (context // CHUNK) + UNROLL
    lanes = local_kv * CHUNK
    dma = pltpu.SemaphoreType.DMA
    hbm = pl.BlockSpec(memory_space=pl.ANY)
    vmem = pl.BlockSpec(memory_space=pltpu.VMEM)
    smem = pl.BlockSpec(memory_space=pltpu.SMEM)
    return pl.pallas_call(
        attend_kernel,
        out_shape=(jax.ShapeDtypeStruct((batch, model_dim), BF16),
                   jax.ShapeDtypeStruct((batch, q_dim), BF16),
                   jax.ShapeDtypeStruct((batch, 2 * local_kv * head_dim), BF16)),
        in_specs=[smem, hbm, vmem, vmem, vmem, hbm, hbm, hbm, hbm, hbm],
        out_specs=(vmem, vmem, vmem),
        scratch_shapes=[
            pltpu.VMEM((batch, model_dim), BF16),
            pltpu.VMEM((q_dim // TILE + 2, model_dim, TILE), BF16),
            pltpu.VMEM((2, GROUP, local_kv, context, head_dim), BF16),
            pltpu.VMEM((2, GROUP, local_kv, context, head_dim), BF16),
            pltpu.VMEM((batch, 8, head_dim), F32),
            pltpu.VMEM((batch, 8, head_dim), F32),
            pltpu.VMEM((batch, 8, head_dim), F32),
            pltpu.VMEM((items, 8, lanes), F32),
            pltpu.VMEM((GROUP + 1, 8, lanes), F32),
            pltpu.VMEM((GROUP + 1, 8, lanes), F32),
            pltpu.VMEM((GROUP + 1, 8, head_dim), F32),
            pltpu.SMEM((2, items), jnp.int32),
            pltpu.SMEM((2, items), jnp.int32),
            pltpu.SMEM((2,), jnp.int32),
            dma, dma((q_dim // TILE + 2,)), dma((2,)), dma((2,)),
        ],
        compiler_params=pltpu.CompilerParams(vmem_limit_bytes=60 * 2 ** 20),
        name="qkv_and_attend",
    )(lengths, tokens, norm_gain.reshape(1, model_dim), cos_part, sin_part, k_cache, v_cache, w_query, w_key, w_value)


def mlp_kernel(h_buf, tokens, o_buf, kv_buf, w_gate, w_up, w_down, w_out,
               y_out, key_out, value_out,
               x_buf, w_buf, wo_buf, u_buf, part, from_sib, to_cross, from_cross, y_buf, kv_in, head_buf, new_buf,
               in_sem, w_sem, wo_sem, kv_send, kv_recv, s1_send, s1_recv, s2_send, s2_recv,
               yc_send, yc_recv, ys_send, ys_recv, yr_send, yr_recv, out_sem, new_sem):
    me = lax.axis_index('model')
    core = lax.rem(me, 2)
    chip = lax.div(me, 2)
    sib = chip * 2 + (1 - core)
    cross = (1 - chip) * 2 + core
    diag = (1 - chip) * 2 + (1 - core)
    model_dim = w_gate.shape[0]
    width = w_gate.shape[1]
    n_hid = width // TILE
    n_out = model_dim // TILE
    head_dim = head_buf.shape[2]
    local_kv = kv_buf.shape[2] // (2 * head_dim)

    barrier = pltpu.get_barrier_semaphore()
    for peer in (sib, cross, diag):
        pl.semaphore_signal(barrier, inc=1, device_id={'model': peer}, device_id_type=MESH)

    def cols(tile):
        return pl.ds(pl.multiple_of(tile * TILE, TILE), TILE)

    def fetch(src, tile, slot):
        return pltpu.make_async_copy(src.at[:, cols(tile)], w_buf.at[slot], w_sem.at[slot])

    def remote(src, dst, send, recv, peer):
        return pltpu.make_async_remote_copy(src_ref=src, dst_ref=dst, send_sem=send, recv_sem=recv,
                                            device_id={'model': peer}, device_id_type=MESH)

    for pair in range(AHEAD):
        fetch(w_gate, pair, 2 * pair).start()
        fetch(w_up, pair, 2 * pair + 1).start()
    x_copy = pltpu.make_async_copy(tokens.at[me], x_buf, in_sem)
    x_copy.start()

    def hidden_tile(j):
        slot = lax.rem(2 * j, SLOTS)
        fetch(w_gate, j, slot).wait()
        gate = jnp.dot(h_buf[...], w_buf[slot], preferred_element_type=F32)
        fetch(w_up, j, slot + 1).wait()
        up = jnp.dot(h_buf[...], w_buf[slot + 1], preferred_element_type=F32)
        u_buf[:, cols(j)] = (jax.nn.silu(gate) * up).astype(BF16)
        return slot

    @pl.loop(0, n_hid - AHEAD)
    def _(j):
        slot = hidden_tile(j)
        fetch(w_gate, j + AHEAD, slot).start()
        fetch(w_up, j + AHEAD, slot + 1).start()

    wo_copy = pltpu.make_async_copy(w_out, wo_buf, wo_sem)
    wo_copy.start()
    pl.semaphore_wait(barrier, 3)
    kv_sends = []
    for n, peer in enumerate((sib, cross, diag)):
        send = remote(kv_buf.at[peer], kv_in.at[me], kv_send.at[n], kv_recv.at[n], peer)
        send.start()
        kv_sends.append(send)

    @pl.loop(n_hid - AHEAD, n_hid)
    def _(j):
        slot = hidden_tile(j)
        tile = 2 * (j - (n_hid - AHEAD))
        fetch(w_down, tile, slot).start()
        fetch(w_down, tile + 1, slot + 1).start()

    x_copy.wait()
    wo_copy.wait()

    def sib_send(c):
        return remote(part.at[c, :, 1 - core], from_sib.at[c], s1_send.at[c], s1_recv.at[c], sib)

    def cross_send(c):
        return remote(to_cross.at[c], from_cross.at[c], s2_send.at[c], s2_recv.at[c], cross)

    def y_cross(c):
        return remote(y_buf.at[c, me], y_buf.at[c, me], yc_send.at[c], yc_recv.at[c], cross)

    def y_sib(c):
        return remote(y_buf.at[c, me], y_buf.at[c, me], ys_send.at[c], ys_recv.at[c], sib)

    def y_relay(c):
        return remote(y_buf.at[c, cross], y_buf.at[c, cross], yr_send.at[c], yr_recv.at[c], sib)

    def y_store(c):
        return pltpu.make_async_copy(y_buf.at[c], y_out.at[:, :, cols(c)], out_sem.at[c])

    @pl.loop(0, n_out + 6)
    def _(i):
        @pl.when(i < n_out)
        def _():
            slot = lax.rem(i, SLOTS)
            fetch(w_down, i, slot).wait()
            total = jnp.dot(u_buf[...], w_buf[slot], preferred_element_type=F32)
            total += jnp.dot(o_buf[...], wo_buf[:, cols(i)], preferred_element_type=F32)
            part[i] = total.reshape(part.shape[1:])
            sib_send(i).start()

        @pl.when(i < n_out - SLOTS)
        def _():
            fetch(w_down, i + SLOTS, lax.rem(i, SLOTS)).start()

        @pl.when((i >= 1) & (i < n_out + 1))
        def _():
            c = i - 1
            sib_send(c).wait_recv()
            to_cross[c] = part[c, 1 - chip, core] + from_sib[c, 1 - chip]
            cross_send(c).start()

        @pl.when((i >= 3) & (i < n_out + 3))
        def _():
            c = i - 3
            cross_send(c).wait_recv()
            total = part[c, chip, core] + from_sib[c, chip] + from_cross[c]
            y_buf[c, me] = (x_buf[:, cols(c)].astype(F32) + total).astype(BF16)
            y_cross(c).start()
            y_sib(c).start()

        @pl.when((i >= 5) & (i < n_out + 5))
        def _():
            c = i - 5
            y_cross(c).wait_recv()
            y_relay(c).start()

        @pl.when(i == n_out)
        def _():
            for send in kv_sends:
                send.wait_recv()
            kv_in[me] = kv_buf[me]
            for half, out in enumerate((key_out, value_out)):
                for source in range(kv_in.shape[0]):
                    for g in range(local_kv):
                        start = (half * local_kv + g) * head_dim
                        head_buf[:, source * local_kv + g, :] = kv_in[source, :, start:start + head_dim].astype(F32)
                new_buf[half] = head_buf[...].astype(BF16)
                pltpu.make_async_copy(new_buf.at[half], out, new_sem.at[half]).start()

        @pl.when(i >= 6)
        def _():
            c = i - 6
            y_sib(c).wait_recv()
            y_relay(c).wait_recv()
            y_store(c).start()

    for send in kv_sends:
        send.wait_send()
    for half, out in enumerate((key_out, value_out)):
        pltpu.make_async_copy(new_buf.at[half], out, new_sem.at[half]).wait()

    @pl.loop(0, n_out)
    def _(c):
        sib_send(c).wait_send()
        cross_send(c).wait_send()
        y_cross(c).wait_send()
        y_sib(c).wait_send()
        y_relay(c).wait_send()
        y_store(c).wait()


def mlp_and_sum(normed, tokens, attended, kv_new, w_gate, w_up, w_down, w_out, kv_heads, head_dim):
    batch, model_dim = normed.shape
    width = w_gate.shape[1]
    q_dim = w_out.shape[0]
    devices = 4
    rows = batch // devices
    n_out = model_dim // TILE
    kv_width = kv_new.shape[1]
    dma = pltpu.SemaphoreType.DMA
    hbm = pl.BlockSpec(memory_space=pl.ANY)
    vmem = pl.BlockSpec(memory_space=pltpu.VMEM)
    out = pl.BlockSpec(memory_space=pltpu.HBM)
    y, key_out, value_out = pl.pallas_call(
        mlp_kernel,
        out_shape=(jax.ShapeDtypeStruct((devices, rows, model_dim), BF16),
                   jax.ShapeDtypeStruct((rows, kv_heads, head_dim), BF16),
                   jax.ShapeDtypeStruct((rows, kv_heads, head_dim), BF16)),
        in_specs=[vmem, hbm, vmem, vmem] + [hbm] * 4,
        out_specs=(out, out, out),
        scratch_shapes=[
            pltpu.VMEM((rows, model_dim), BF16),
            pltpu.VMEM((SLOTS, model_dim, TILE), BF16),
            pltpu.VMEM((q_dim, model_dim), BF16),
            pltpu.VMEM((batch, width), BF16),
            pltpu.VMEM((n_out, 2, 2, rows, TILE), F32),
            pltpu.VMEM((n_out, 2, rows, TILE), F32),
            pltpu.VMEM((n_out, rows, TILE), F32),
            pltpu.VMEM((n_out, rows, TILE), F32),
            pltpu.VMEM((n_out, devices, rows, TILE), BF16),
            pltpu.VMEM((devices, rows, kv_width), BF16),
            pltpu.VMEM((rows, kv_heads, head_dim), F32),
            pltpu.VMEM((2, rows, kv_heads, head_dim), BF16),
            dma, dma((SLOTS,)), dma, dma((3,)), dma((3,)),
        ] + [dma((n_out,))] * 11 + [dma((2,))],
        compiler_params=pltpu.CompilerParams(collective_id=0, has_side_effects=True, vmem_limit_bytes=48 * 2 ** 20),
        name="mlp_and_sum",
    )(normed, tokens.reshape(devices, rows, model_dim), attended, kv_new.reshape(devices, rows, kv_width), w_gate, w_up, w_down, w_out)
    return y.reshape(batch, model_dim), key_out, value_out


def solution(mesh):
    groups = mesh.shape['model']

    def local_step(tokens, lengths, k_cache, v_cache, norm_gain, w_query, w_key, w_value, w_out, w_gate, w_up, w_down):
        kv_heads, _, head_dim = k_cache.shape[1:]
        normed, attended, kv_new = qkv_and_attend(tokens, lengths, k_cache, v_cache, norm_gain, w_query, w_key, w_value, groups)
        return mlp_and_sum(normed, tokens, attended, kv_new, w_gate, w_up, w_down, w_out, kv_heads, head_dim)

    in_specs = (P('replica', None), P('replica'), P('replica', None, None, None), P('replica', None, None, None), P(None), P(None, 'model'), P(None, None), P(None, None), P('model', None), P(None, 'model'), P(None, 'model'), P('model', None))
    out_specs = (P('replica', None), P(('replica', 'model'), None, None), P(('replica', 'model'), None, None))
    return jax.shard_map(local_step, mesh=mesh, in_specs=in_specs, out_specs=out_specs, check_vma=False)
```

```python
import functools
import math

import jax
import jax.numpy as jnp
import numpy as np
from jax import lax
from jax.experimental import pallas as pl
from jax.experimental.pallas import tpu as pltpu
from jax.sharding import PartitionSpec as P

ROPE_BASE = 10000.0
NORM_EPS = 1e-6
MASK_VALUE = -1e30
MESH = pl.DeviceIdType.MESH
F32 = jnp.float32
BF16 = jnp.bfloat16
TILE = 256
SLOTS = 12
LAGS = (1, 6, 11, 13)
CHUNK = 64
UNROLL = 16
FRONT_VMEM = 52 * 2 ** 20
BACK_VMEM = 44 * 2 ** 20
RING = 256


def front_kernel(lengths, tokens, gain, freq, k_cache, v_cache, w_query, w_key, w_value, w_gate, w_up,
                 o_out, kv_out, u_out,
                 x_buf, h_buf, w_buf, k_ring, v_ring, q_buf, kn_buf, vn_buf, pair_buf, score, peak, total, mixed, angle, rot,
                 item_seq, item_pos, x_sem, w_sem, k_sem, v_sem):
    batch, model_dim = tokens.shape
    head_dim = freq.shape[1]
    local_kv = kv_out.shape[1] // (2 * head_dim)
    heads = o_out.shape[1] // head_dim
    ratio = heads // local_kv
    q_tiles = w_query.shape[1] // TILE
    lead = q_tiles + 2
    pieces = 2 * w_gate.shape[1] // TILE
    ring_steps = RING // UNROLL
    scale = head_dim ** -0.5
    me = lax.axis_index('model')
    first_kv = me * local_kv

    def cols(tile):
        return pl.ds(pl.multiple_of(tile * TILE, TILE), TILE)

    def w_copy(src, tile, t):
        slot = t % SLOTS
        return pltpu.make_async_copy(src.at[:, cols(tile)], w_buf.at[slot], w_sem.at[slot])

    x_copy = pltpu.make_async_copy(tokens, x_buf, x_sem)
    x_copy.start()
    lead_copies = [w_copy(w_key, me, 0), w_copy(w_value, me, 1)] + [w_copy(w_query, t, 2 + t) for t in range(q_tiles)]
    for copy in lead_copies:
        copy.start()

    def row_copy(cache, ring, sem, k):
        slot = lax.rem(k, RING)
        seq = lax.rem(item_seq[k], batch)
        return pltpu.make_async_copy(cache.at[seq, pl.ds(first_kv, local_kv), pl.ds(pl.multiple_of(item_pos[k], CHUNK), CHUNK)],
                                     ring.at[slot], sem.at[lax.div(slot, UNROLL)])

    def list_seq(seq, k):
        def list_item(c, k):
            item_seq[k] = seq
            item_pos[k] = c * CHUNK

            @pl.when(k < RING)
            def _():
                row_copy(k_cache, k_ring, k_sem, k).start()

            return k + 1

        return lax.fori_loop(0, lax.div(lengths[seq] + (CHUNK - 1), CHUNK), list_item, k)

    n_items = lax.fori_loop(0, batch, list_seq, 0)
    steps = lax.div(n_items + (UNROLL - 1), UNROLL)

    @pl.loop(n_items, steps * UNROLL)
    def _(k):
        item_seq[k] = batch
        item_pos[k] = 0

        @pl.when(k < RING)
        def _():
            row_copy(k_cache, k_ring, k_sem, k).start()

    def piece_copy(p):
        return w_copy((w_gate, w_up)[p % 2], p // 2, lead + p)

    for p in range(SLOTS - lead):
        piece_copy(p).start()

    @pl.loop(0, jnp.minimum(steps * UNROLL, RING))
    def _(k):
        row_copy(v_cache, v_ring, v_sem, k).start()

    @pl.loop(0, batch // 8)
    def _(i):
        for r in range(8):
            angle[pl.ds(i * 8 + r, 1), :] = lengths[i * 8 + r].astype(F32) * freq[...]

    first = lax.broadcasted_iota(jnp.int32, (batch, head_dim), 1) < head_dim // 2
    rot[0] = jnp.cos(angle[...])
    rot[1] = jnp.where(first, -jnp.sin(angle[...]), jnp.sin(angle[...]))

    x_copy.wait()
    x = x_buf[...].astype(F32)
    mean_sq = jnp.mean(x * x, axis=-1, keepdims=True)
    h_buf[...] = (x * lax.rsqrt(mean_sq + NORM_EPS) * gain[...].reshape(1, model_dim).astype(F32)).astype(BF16)

    def rope(a):
        return a * rot[0] + pltpu.roll(a, head_dim // 2, 1) * rot[1]

    for t, copy in enumerate(lead_copies):
        copy.wait()
        prod = jnp.dot(h_buf[...], w_buf[t], preferred_element_type=F32)
        if t + SLOTS - lead < pieces:
            piece_copy(t + SLOTS - lead).start()
        for j in range(TILE // head_dim):
            a = prod[:, j * head_dim:(j + 1) * head_dim]
            if t >= 2:
                q_buf[:, (t - 2) * (TILE // head_dim) + j, :] = rope(a).astype(BF16).astype(F32)
            else:
                a = (rope(a) if t == 0 else a).astype(BF16)
                col = (t * local_kv + j) * head_dim
                kv_out[:, col:col + head_dim] = a
                (kn_buf, vn_buf)[t][j] = a.astype(F32)
    for h in range(heads, q_buf.shape[1]):
        q_buf[:, h, :] = jnp.zeros((batch, head_dim), F32)
    peak[...] = jnp.full(peak.shape, MASK_VALUE, F32)
    total[...] = jnp.zeros(total.shape, F32)
    mixed[...] = jnp.zeros(mixed.shape, F32)

    sub = q_buf.shape[1]
    lane = lax.broadcasted_iota(jnp.int32, (sub, local_kv * CHUNK), 1)
    head = lax.broadcasted_iota(jnp.int32, (sub, local_kv * CHUNK), 0)
    own = (lax.div(lane, CHUNK) == lax.div(head, ratio)) & (head < heads)
    pos_in = jnp.where(own, lax.rem(lane, CHUNK), 1 << 20)

    def wait_step(cache, ring, sem, step):
        at = lax.rem(step, ring_steps)
        pltpu.make_async_copy(ring.at[pl.ds(0, UNROLL)], ring.at[pl.ds(at * UNROLL, UNROLL)], sem.at[at]).wait()

    def refill(cache, ring, sem, step):
        @pl.when(step + ring_steps < steps)
        def _():
            @pl.loop(0, UNROLL)
            def _(u):
                row_copy(cache, ring, sem, (step + ring_steps) * UNROLL + u).start()

    def score_step(step):
        base = lax.rem(step, ring_steps) * UNROLL
        found = []
        for u in range(UNROLL):
            k = step * UNROLL + u
            seq = item_seq[k]
            row = lax.rem(seq, batch)
            keys = k_ring[base + u].reshape(local_kv * CHUNK, head_dim)
            s = lax.dot_general(q_buf[row].astype(BF16), keys, (((1,), (1,)), ((), ())), preferred_element_type=F32) * scale
            s = jnp.where(pos_in < lengths[row] - item_pos[k], s, MASK_VALUE)
            score[k] = s
            found.append((seq, s))
        for seq, s in found:
            peak[seq] = jnp.maximum(peak[seq], s)

    def value_step(step):
        base = lax.rem(step, ring_steps) * UNROLL
        found = []
        for u in range(UNROLL):
            k = step * UNROLL + u
            seq = item_seq[k]
            p = jnp.exp(score[k] - peak[seq])
            values = v_ring[base + u].reshape(local_kv * CHUNK, head_dim)
            found.append((seq, p, jnp.dot(p.astype(BF16), values, preferred_element_type=F32)))
        for seq, p, o in found:
            total[seq] = total[seq] + p
            mixed[seq] = mixed[seq] + o

    def wait_piece(p):
        slot = lax.rem(lead + p, SLOTS)
        pltpu.make_async_copy(w_gate.at[:, cols(0)], w_buf.at[slot], w_sem.at[slot]).wait()

    def piece(p):
        prod = jnp.dot(h_buf[...], w_buf[lax.rem(lead + p, SLOTS)], preferred_element_type=F32)
        pair_buf[lax.rem(p, 2)] = prod
        u_out[:, cols(lax.div(p, 2))] = (jax.nn.silu(pair_buf[0]) * pair_buf[1]).astype(BF16)

    def next_piece(p):
        slot = lax.rem(lead + p, SLOTS)
        later = p + SLOTS
        for parity, src in enumerate((w_gate, w_up)):
            @pl.when((later < pieces) & (lax.rem(p, 2) == parity))
            def _():
                pltpu.make_async_copy(src.at[:, cols(lax.div(later, 2))], w_buf.at[slot], w_sem.at[slot]).start()

    def both(attend_step, cache, ring, sem, p0, p1):
        fused = jnp.minimum(steps, p1 - p0)

        @pl.loop(0, fused)
        def _(s):
            wait_step(cache, ring, sem, s)
            wait_piece(p0 + s)
            attend_step(s)
            piece(p0 + s)
            refill(cache, ring, sem, s)
            next_piece(p0 + s)

        @pl.loop(fused, steps)
        def _(s):
            wait_step(cache, ring, sem, s)
            attend_step(s)
            refill(cache, ring, sem, s)

        @pl.loop(p0 + fused, p1)
        def _(p):
            wait_piece(p)
            piece(p)
            next_piece(p)

    both(score_step, k_cache, k_ring, k_sem, 0, pieces // 2)

    def new_score(h):
        return jnp.sum(q_buf[:, h, :] * kn_buf[h // ratio], axis=-1, keepdims=True) * scale

    for h in range(heads):
        top = jnp.maximum(jnp.max(peak[:batch, h, :], axis=-1, keepdims=True), new_score(h))
        peak[:batch, h, :] = jnp.broadcast_to(top, (batch, peak.shape[2]))

    both(value_step, v_cache, v_ring, v_sem, pieces // 2, pieces)

    for h in range(heads):
        weight_new = jnp.exp(new_score(h) - peak[:batch, h, :1])
        norm = jnp.sum(total[:batch, h, :], axis=-1, keepdims=True) + weight_new
        out = mixed[:batch, h, :] + weight_new.astype(BF16).astype(F32) * vn_buf[h // ratio]
        o_out[:, h * head_dim:(h + 1) * head_dim] = (out / norm).astype(BF16)


def front(tokens, lengths, k_cache, v_cache, norm_gain, w_query, w_key, w_value, w_gate, w_up, groups):
    batch, model_dim = tokens.shape
    kv_heads, context, head_dim = k_cache.shape[1:]
    local_kv = kv_heads // groups
    q_dim = w_query.shape[1]
    width = w_gate.shape[1]
    half_freq = np.exp(np.arange(head_dim // 2) * (-2.0 * math.log(ROPE_BASE) / head_dim))
    freq = jnp.asarray(np.concatenate([half_freq, half_freq])[None, :], F32)
    items = batch * (context // CHUNK) + UNROLL
    lanes = local_kv * CHUNK
    dma = pltpu.SemaphoreType.DMA
    hbm = pl.BlockSpec(memory_space=pl.ANY)
    vmem = pl.BlockSpec(memory_space=pltpu.VMEM)
    smem = pl.BlockSpec(memory_space=pltpu.SMEM)
    return pl.pallas_call(
        front_kernel,
        out_shape=(jax.ShapeDtypeStruct((batch, q_dim), BF16),
                   jax.ShapeDtypeStruct((batch, 2 * local_kv * head_dim), BF16),
                   jax.ShapeDtypeStruct((batch, width), BF16)),
        in_specs=[smem, hbm, vmem, vmem] + [hbm] * 7,
        out_specs=(vmem, vmem, vmem),
        scratch_shapes=[
            pltpu.VMEM((batch, model_dim), BF16),
            pltpu.VMEM((batch, model_dim), BF16),
            pltpu.VMEM((SLOTS, model_dim, TILE), BF16),
            pltpu.VMEM((RING, local_kv, CHUNK, head_dim), BF16),
            pltpu.VMEM((RING, local_kv, CHUNK, head_dim), BF16),
            pltpu.VMEM((batch, 8, head_dim), F32),
            pltpu.VMEM((local_kv, batch, head_dim), F32),
            pltpu.VMEM((local_kv, batch, head_dim), F32),
            pltpu.VMEM((2, batch, TILE), F32),
            pltpu.VMEM((items, 8, lanes), F32),
            pltpu.VMEM((batch + 1, 8, lanes), F32),
            pltpu.VMEM((batch + 1, 8, lanes), F32),
            pltpu.VMEM((batch + 1, 8, head_dim), F32),
            pltpu.VMEM((batch, head_dim), F32),
            pltpu.VMEM((2, batch, head_dim), F32),
            pltpu.SMEM((items,), jnp.int32),
            pltpu.SMEM((items,), jnp.int32),
            dma, dma((SLOTS,)), dma((RING // UNROLL,)), dma((RING // UNROLL,)),
        ],
        compiler_params=pltpu.CompilerParams(vmem_limit_bytes=FRONT_VMEM),
        name="front",
    )(lengths, tokens, norm_gain, freq, k_cache, v_cache, w_query, w_key, w_value, w_gate, w_up)


def back_kernel(u_buf, tokens, o_buf, kv_buf, w_down, w_out,
                y_out, key_out, value_out,
                x_buf, w_buf, wo_buf, part, from_sib, to_cross, from_cross, y_buf, kv_in, head_buf,
                in_sem, w_sem, wo_sem, kv_send, kv_recv, s1_send, s1_recv, s2_send, s2_recv,
                yc_send, yc_recv, ys_send, ys_recv, yr_send, yr_recv):
    me = lax.axis_index('model')
    core = lax.rem(me, 2)
    chip = lax.div(me, 2)
    sib = chip * 2 + (1 - core)
    cross = (1 - chip) * 2 + core
    diag = (1 - chip) * 2 + (1 - core)
    n_out = w_down.shape[1] // TILE
    head_dim = head_buf.shape[2]
    local_kv = kv_buf.shape[2] // (2 * head_dim)
    lag_sib, lag_cross, lag_relay, lag_store = LAGS

    barrier = pltpu.get_barrier_semaphore()
    for peer in (sib, cross, diag):
        pl.semaphore_signal(barrier, inc=1, device_id={'model': peer}, device_id_type=MESH)

    def cols(tile):
        return pl.ds(pl.multiple_of(tile * TILE, TILE), TILE)

    def down_copy(c):
        return pltpu.make_async_copy(w_down.at[:, cols(c)], w_buf.at[c], w_sem.at[c])

    def out_copy(c):
        return pltpu.make_async_copy(w_out.at[:, cols(c)], wo_buf.at[c], wo_sem.at[c])

    def remote(src, dst, send, recv, peer):
        return pltpu.make_async_remote_copy(src_ref=src, dst_ref=dst, send_sem=send, recv_sem=recv,
                                            device_id={'model': peer}, device_id_type=MESH)

    @pl.loop(0, n_out)
    def _(c):
        out_copy(c).start()
        down_copy(c).start()

    x_copy = pltpu.make_async_copy(tokens.at[me], x_buf, in_sem)
    x_copy.start()
    pl.semaphore_wait(barrier, 3)
    kv_sends = []
    for n, peer in enumerate((sib, cross, diag)):
        send = remote(kv_buf.at[peer], kv_in.at[me], kv_send.at[n], kv_recv.at[n], peer)
        send.start()
        kv_sends.append(send)
    x_copy.wait()

    def sib_send(c):
        return remote(part.at[c, :, 1 - core], from_sib.at[c], s1_send.at[c], s1_recv.at[c], sib)

    def cross_send(c):
        return remote(to_cross.at[c], from_cross.at[c], s2_send.at[c], s2_recv.at[c], cross)

    def y_cross(c):
        return remote(y_buf.at[c, me], y_buf.at[c, me], yc_send.at[c], yc_recv.at[c], cross)

    def y_sib(c):
        return remote(y_buf.at[c, me], y_buf.at[c, me], ys_send.at[c], ys_recv.at[c], sib)

    def y_relay(c):
        return remote(y_buf.at[c, cross], y_buf.at[c, cross], yr_send.at[c], yr_recv.at[c], sib)

    @pl.loop(0, n_out + lag_store)
    def _(i):
        @pl.when(i < n_out)
        def _():
            out_copy(i).wait()
            total = jnp.dot(o_buf[...], wo_buf[i], preferred_element_type=F32)
            down_copy(i).wait()
            total += jnp.dot(u_buf[...], w_buf[i], preferred_element_type=F32)
            part[i] = total.reshape(part.shape[1:])
            sib_send(i).start()

        @pl.when((i >= lag_sib) & (i < n_out + lag_sib))
        def _():
            c = i - lag_sib
            sib_send(c).wait_recv()
            to_cross[c] = part[c, 1 - chip, core] + from_sib[c, 1 - chip]
            cross_send(c).start()

        @pl.when((i >= lag_cross) & (i < n_out + lag_cross))
        def _():
            c = i - lag_cross
            cross_send(c).wait_recv()
            total = part[c, chip, core] + from_sib[c, chip] + from_cross[c]
            y_buf[c, me] = (x_buf[:, cols(c)].astype(F32) + total).astype(BF16)
            y_cross(c).start()
            y_sib(c).start()

        @pl.when((i >= lag_relay) & (i < n_out + lag_relay))
        def _():
            c = i - lag_relay
            y_cross(c).wait_recv()
            y_relay(c).start()

        @pl.when(i == n_out)
        def _():
            for send in kv_sends:
                send.wait_recv()
            kv_in[me] = kv_buf[me]
            for half, out in enumerate((key_out, value_out)):
                for source in range(kv_in.shape[0]):
                    for g in range(local_kv):
                        start = (half * local_kv + g) * head_dim
                        head_buf[:, source * local_kv + g, :] = kv_in[source, :, start:start + head_dim].astype(F32)
                out[...] = head_buf[...].astype(BF16)

        @pl.when(i >= lag_store)
        def _():
            c = i - lag_store
            y_sib(c).wait_recv()
            y_relay(c).wait_recv()
            y_out[:, :, cols(c)] = y_buf[c]

    for send in kv_sends:
        send.wait_send()

    @pl.loop(0, n_out)
    def _(c):
        sib_send(c).wait_send()
        cross_send(c).wait_send()
        y_cross(c).wait_send()
        y_sib(c).wait_send()
        y_relay(c).wait_send()


def back(hidden, tokens, attended, kv_new, w_down, w_out, kv_heads, head_dim):
    batch, model_dim = tokens.shape
    width = w_down.shape[0]
    q_dim = w_out.shape[0]
    devices = 4
    rows = batch // devices
    n_out = model_dim // TILE
    kv_width = kv_new.shape[1]
    dma = pltpu.SemaphoreType.DMA
    hbm = pl.BlockSpec(memory_space=pl.ANY)
    vmem = pl.BlockSpec(memory_space=pltpu.VMEM)
    y, key_out, value_out = pl.pallas_call(
        back_kernel,
        out_shape=(jax.ShapeDtypeStruct((devices, rows, model_dim), BF16),
                   jax.ShapeDtypeStruct((rows, kv_heads, head_dim), BF16),
                   jax.ShapeDtypeStruct((rows, kv_heads, head_dim), BF16)),
        in_specs=[vmem, hbm, vmem, vmem, hbm, hbm],
        out_specs=(vmem, vmem, vmem),
        scratch_shapes=[
            pltpu.VMEM((rows, model_dim), BF16),
            pltpu.VMEM((n_out, width, TILE), BF16),
            pltpu.VMEM((n_out, q_dim, TILE), BF16),
            pltpu.VMEM((n_out, 2, 2, rows, TILE), F32),
            pltpu.VMEM((n_out, 2, rows, TILE), F32),
            pltpu.VMEM((n_out, rows, TILE), F32),
            pltpu.VMEM((n_out, rows, TILE), F32),
            pltpu.VMEM((n_out, devices, rows, TILE), BF16),
            pltpu.VMEM((devices, rows, kv_width), BF16),
            pltpu.VMEM((rows, kv_heads, head_dim), F32),
            dma, dma((n_out,)), dma((n_out,)), dma((3,)), dma((3,)),
        ] + [dma((n_out,))] * 10,
        compiler_params=pltpu.CompilerParams(collective_id=0, has_side_effects=True, vmem_limit_bytes=BACK_VMEM),
        name="back",
    )(hidden, tokens.reshape(devices, rows, model_dim), attended, kv_new.reshape(devices, rows, kv_width), w_down, w_out)
    return y.reshape(batch, model_dim), key_out, value_out


def solution(mesh):
    groups = mesh.shape['model']

    def local_step(tokens, lengths, k_cache, v_cache, norm_gain, w_query, w_key, w_value, w_out, w_gate, w_up, w_down):
        kv_heads, _, head_dim = k_cache.shape[1:]
        attended, kv_new, hidden = front(tokens, lengths, k_cache, v_cache, norm_gain, w_query, w_key, w_value, w_gate, w_up, groups)
        return back(hidden, tokens, attended, kv_new, w_down, w_out, kv_heads, head_dim)

    in_specs = (P('replica', None), P('replica'), P('replica', None, None, None), P('replica', None, None, None), P(None), P(None, 'model'), P(None, None), P(None, None), P('model', None), P(None, 'model'), P(None, 'model'), P('model', None))
    out_specs = (P('replica', None), P(('replica', 'model'), None, None), P(('replica', 'model'), None, None))
    return jax.shard_map(local_step, mesh=mesh, in_specs=in_specs, out_specs=out_specs, check_vma=False)
```

```python
import functools
import math

import jax
import jax.numpy as jnp
import numpy as np
from jax import lax
from jax.experimental import pallas as pl
from jax.experimental.pallas import tpu as pltpu
from jax.sharding import PartitionSpec as P

ROPE_BASE = 10000.0
NORM_EPS = 1e-6
MASK_VALUE = -1e30
MESH = pl.DeviceIdType.MESH
F32 = jnp.float32
BF16 = jnp.bfloat16
TILE = 256
SLOTS = 12
LAGS = (1, 6, 11, 13)
CHUNK = 64
UNROLL = 16
VMEM_BYTES = 67_043_328
RESULT_BYTES = 950_000
PIECES_SCORE = 12
PIECES_VALUE = 11
RING = 256


def front_kernel(lengths, tokens, gain_hbm, freq_hbm, k_cache, v_cache, w_query, w_key, w_value, w_gate, w_up,
                 o_hbm, kv_hbm, u_hbm,
                 x_buf, h_buf, w_buf, k_ring, v_ring, q_buf, kn_buf, vn_buf, fresh, score, peak, total, mixed, angle, rot,
                 gain, freq, o_out, kv_out, u_out,
                 item_seq, item_pos, out_sem, x_sem, w_sem, k_sem, v_sem):
    batch, model_dim = tokens.shape
    head_dim = freq.shape[1]
    local_kv = kv_out.shape[1] // (2 * head_dim)
    heads = o_out.shape[1] // head_dim
    ratio = heads // local_kv
    q_tiles = w_query.shape[1] // TILE
    lead = q_tiles + 2
    half = TILE // 2
    pieces = w_gate.shape[1] // half
    ring_steps = RING // UNROLL
    first_steps = batch // UNROLL
    scale = head_dim ** -0.5
    me = lax.axis_index('model')
    local = pl.ds(me * local_kv, local_kv)
    lanes = local_kv * CHUNK

    def w_copy(src, tile, t):
        return pltpu.make_async_copy(src.at[:, pl.ds(pl.multiple_of(tile * TILE, TILE), TILE)], w_buf.at[t], w_sem.at[t])

    def start_piece(p, slot):
        for n, src in enumerate((w_gate, w_up)):
            pltpu.make_async_copy(src.at[:, pl.ds(pl.multiple_of(p * half, half), half)],
                                  w_buf.at[slot, :, n * half:(n + 1) * half], w_sem.at[slot]).start()

    def first_copy(cache, ring, sem, step):
        rows = pl.ds(step * UNROLL, UNROLL)
        return pltpu.make_async_copy(cache.at[rows, local, pl.ds(0, CHUNK)], ring.at[rows], sem.at[step])

    def item_copy(cache, ring, sem, k):
        slot = lax.rem(k, RING)
        return pltpu.make_async_copy(cache.at[lax.rem(item_seq[k], batch), local, pl.ds(pl.multiple_of(item_pos[k], CHUNK), CHUNK)],
                                     ring.at[slot], sem.at[lax.div(slot, UNROLL)])

    x_copy = pltpu.make_async_copy(tokens, x_buf, x_sem.at[0])
    gain_copy = pltpu.make_async_copy(gain_hbm, gain, x_sem.at[1])
    freq_copy = pltpu.make_async_copy(freq_hbm, freq, x_sem.at[2])
    for copy in (freq_copy, x_copy, gain_copy):
        copy.start()
    lead_copies = [w_copy(w_key, me, 0), w_copy(w_value, me, 1)] + [w_copy(w_query, t, 2 + t) for t in range(q_tiles)]
    for copy in lead_copies:
        copy.start()
    for step in range(first_steps):
        first_copy(k_cache, k_ring, k_sem, step).start()
    for p in range(SLOTS - lead):
        start_piece(p, lead + p)
    for step in range(first_steps):
        first_copy(v_cache, v_ring, v_sem, step).start()

    def second(i, k):
        for r in range(UNROLL):
            seq = i * UNROLL + r
            item_seq[k] = seq
            item_pos[k] = CHUNK
            k = k + (lengths[seq] > CHUNK).astype(jnp.int32)
        return k

    begin = batch
    end = lax.fori_loop(0, batch // UNROLL, second, batch)
    for c in range(2, k_cache.shape[2] // CHUNK):
        def further(i, k):
            seq = item_seq[i]
            item_seq[k] = seq
            item_pos[k] = c * CHUNK
            return k + (lengths[seq] > c * CHUNK).astype(jnp.int32)

        begin, end = end, lax.fori_loop(begin, end, further, end)
    steps = lax.div(end + (UNROLL - 1), UNROLL)

    @pl.loop(end, steps * UNROLL)
    def _(k):
        item_seq[k] = batch
        item_pos[k] = 0

    @pl.loop(batch, jnp.minimum(steps * UNROLL, RING))
    def _(k):
        item_copy(k_cache, k_ring, k_sem, k).start()
        item_copy(v_cache, v_ring, v_sem, k).start()

    freq_copy.wait()

    @pl.loop(0, batch // 8)
    def _(i):
        for r in range(8):
            angle[pl.ds(i * 8 + r, 1), :] = lengths[i * 8 + r].astype(F32) * freq[...]

    first = lax.broadcasted_iota(jnp.int32, (batch, head_dim), 1) < head_dim // 2
    rot[0] = jnp.cos(angle[...])
    rot[1] = jnp.where(first, -jnp.sin(angle[...]), jnp.sin(angle[...]))
    q_buf[...] = jnp.zeros(q_buf.shape, F32)

    x_copy.wait()
    gain_copy.wait()
    x = x_buf[...].astype(F32)
    mean_sq = jnp.mean(x * x, axis=-1, keepdims=True)
    h_buf[...] = (x * lax.rsqrt(mean_sq + NORM_EPS) * gain[...].reshape(1, model_dim).astype(F32)).astype(BF16)

    def rope(a):
        return a * rot[0] + pltpu.roll(a, head_dim // 2, 1) * rot[1]

    for t, copy in enumerate(lead_copies):
        copy.wait()
        prod = jnp.dot(h_buf[...], w_buf[t], preferred_element_type=F32)
        if SLOTS - lead + t < pieces:
            start_piece(SLOTS - lead + t, t)
        for j in range(TILE // head_dim):
            a = prod[:, j * head_dim:(j + 1) * head_dim]
            if t >= 2:
                q_buf[:, (t - 2) * (TILE // head_dim) + j, :] = rope(a).astype(BF16).astype(F32)
            else:
                a = (rope(a) if t == 0 else a).astype(BF16)
                col = (t * local_kv + j) * head_dim
                kv_out[:, col:col + head_dim] = a
                (kn_buf, vn_buf)[t][j] = a
    kv_copy = pltpu.make_async_copy(kv_out, kv_hbm, out_sem.at[0])
    kv_copy.start()
    peak[batch] = jnp.full(peak.shape[1:], MASK_VALUE, F32)
    total[batch] = jnp.zeros(total.shape[1:], F32)
    mixed[batch] = jnp.zeros(mixed.shape[1:], F32)

    sub = q_buf.shape[1]
    lane = lax.broadcasted_iota(jnp.int32, (sub, lanes), 1)
    head = lax.broadcasted_iota(jnp.int32, (sub, lanes), 0)
    own = (lax.div(lane, CHUNK) == lax.div(head, ratio)) & (head < heads)
    pos_in = jnp.where(own, lax.rem(lane, CHUNK), 1 << 20)

    line = lax.broadcasted_iota(jnp.int32, (CHUNK, sub, lanes), 0)
    mine = line == pos_in[None]
    blocks = [slice(b0, b0 + CHUNK) for b0 in range(0, batch, CHUNK)]
    for rows in blocks:
        q = q_buf[rows].reshape(CHUNK * sub, head_dim).astype(BF16)
        s = lax.dot_general(q, kn_buf[:, rows].reshape(lanes, head_dim), (((1,), (1,)), ((), ())), preferred_element_type=F32) * scale
        s = jnp.where(mine, s.reshape(CHUNK, sub, lanes), MASK_VALUE)
        fresh[rows] = s
        peak[rows] = s

    def wait_step(ring, sem, step):
        at = lax.rem(step, ring_steps)
        pltpu.make_async_copy(ring.at[pl.ds(0, UNROLL)], ring.at[pl.ds(at * UNROLL, UNROLL)], sem.at[at]).wait()

    def refill(cache, ring, sem, step):
        @pl.when(step + ring_steps < steps)
        def _():
            @pl.loop(0, UNROLL)
            def _(u):
                item_copy(cache, ring, sem, (step + ring_steps) * UNROLL + u).start()

    def item(step, u, listed):
        k = step * UNROLL + u
        if listed:
            return k, item_seq[k], lax.rem(item_seq[k], batch), item_pos[k]
        return k, k, k, 0

    def score_step(step, listed):
        base = lax.rem(step, ring_steps) * UNROLL
        found = []
        for u in range(UNROLL):
            k, seq, row, pos = item(step, u, listed)
            keys = k_ring[base + u].reshape(lanes, head_dim)
            s = lax.dot_general(q_buf[row].astype(BF16), keys, (((1,), (1,)), ((), ())), preferred_element_type=F32) * scale
            s = jnp.where(pos_in < lengths[row] - pos, s, MASK_VALUE)
            score[k] = s
            found.append((seq, s))
        for seq, s in found:
            peak[seq] = jnp.maximum(peak[seq], s)

    def value_step(step, listed):
        base = lax.rem(step, ring_steps) * UNROLL
        found = []
        for u in range(UNROLL):
            k, seq, row, pos = item(step, u, listed)
            p = jnp.exp(score[k] - peak[seq])
            values = v_ring[base + u].reshape(lanes, head_dim)
            found.append((seq, p, jnp.dot(p.astype(BF16), values, preferred_element_type=F32)))
        for seq, p, o in found:
            total[seq] = total[seq] + p
            mixed[seq] = mixed[seq] + o

    def u_copy(p):
        cols = pl.ds(pl.multiple_of(p * half, half), half)
        return pltpu.make_async_copy(u_out.at[:, cols], u_hbm.at[:, cols], out_sem.at[1])

    def wait_piece(p):
        slot = lax.rem(lead + p, SLOTS)
        pltpu.make_async_copy(w_gate.at[:, pl.ds(0, TILE)], w_buf.at[slot], w_sem.at[slot]).wait()

    def piece(p):
        prod = jnp.dot(h_buf[...], w_buf[lax.rem(lead + p, SLOTS)], preferred_element_type=F32)
        u_out[:, pl.ds(pl.multiple_of(p * half, half), half)] = (jax.nn.silu(prod[:, :half]) * prod[:, half:]).astype(BF16)

    def after_piece(p):
        u_copy(p).start()

        @pl.when(p + SLOTS < pieces)
        def _():
            start_piece(p + SLOTS, lax.rem(lead + p, SLOTS))

    def both(attend_step, cache, ring, sem, p0, p1):
        @pl.loop(0, first_steps)
        def _(s):
            wait_step(ring, sem, s)
            wait_piece(p0 + s)
            attend_step(s, False)
            piece(p0 + s)
            refill(cache, ring, sem, s)
            after_piece(p0 + s)

        fused = jnp.minimum(steps, p1 - p0)

        @pl.loop(first_steps, fused)
        def _(s):
            wait_step(ring, sem, s)
            wait_piece(p0 + s)
            attend_step(s, True)
            piece(p0 + s)
            refill(cache, ring, sem, s)
            after_piece(p0 + s)

        @pl.loop(fused, steps)
        def _(s):
            wait_step(ring, sem, s)
            attend_step(s, True)
            refill(cache, ring, sem, s)

        return p0 + fused

    reached = both(score_step, k_cache, k_ring, k_sem, 0, PIECES_SCORE)

    @pl.loop(reached, PIECES_SCORE)
    def _(p):
        wait_piece(p)
        piece(p)
        after_piece(p)

    for rows in blocks:
        top = jnp.broadcast_to(jnp.max(peak[rows], axis=-1, keepdims=True), (CHUNK, sub, lanes))
        peak[rows] = top
        p = jnp.exp(fresh[rows] - top)
        total[rows] = p
        o = jnp.dot(p.reshape(CHUNK * sub, lanes).astype(BF16), vn_buf[:, rows].reshape(lanes, head_dim), preferred_element_type=F32)
        mixed[rows] = o.reshape(CHUNK, sub, head_dim)

    reached = both(value_step, v_cache, v_ring, v_sem, PIECES_SCORE, PIECES_SCORE + PIECES_VALUE)

    q_buf[...] = mixed[:batch] / jnp.sum(total[:batch], axis=-1, keepdims=True)
    for h in range(heads):
        o_out[:, h * head_dim:(h + 1) * head_dim] = q_buf[:, h, :].astype(BF16)
    o_copy = pltpu.make_async_copy(o_out, o_hbm, out_sem.at[2])
    o_copy.start()

    @pl.loop(reached, pieces)
    def _(p):
        wait_piece(p)
        piece(p)
        after_piece(p)

    kv_copy.wait()
    o_copy.wait()
    pltpu.make_async_copy(u_out, u_hbm, out_sem.at[1]).wait()


def front(tokens, lengths, k_cache, v_cache, norm_gain, w_query, w_key, w_value, w_gate, w_up, groups):
    batch, model_dim = tokens.shape
    kv_heads, context, head_dim = k_cache.shape[1:]
    local_kv = kv_heads // groups
    q_dim = w_query.shape[1]
    width = w_gate.shape[1]
    half_freq = np.exp(np.arange(head_dim // 2) * (-2.0 * math.log(ROPE_BASE) / head_dim))
    freq = jnp.asarray(np.concatenate([half_freq, half_freq])[None, :], F32)
    items = batch * (context // CHUNK) + UNROLL
    lanes = local_kv * CHUNK
    dma = pltpu.SemaphoreType.DMA
    hbm = pl.BlockSpec(memory_space=pltpu.HBM)
    smem = pl.BlockSpec(memory_space=pltpu.SMEM)
    return pl.pallas_call(
        front_kernel,
        out_shape=(jax.ShapeDtypeStruct((batch, q_dim), BF16),
                   jax.ShapeDtypeStruct((batch, 2 * local_kv * head_dim), BF16),
                   jax.ShapeDtypeStruct((batch, width), BF16)),
        in_specs=[smem] + [hbm] * 10,
        out_specs=(hbm, hbm, hbm),
        scratch_shapes=[
            pltpu.VMEM((batch, model_dim), BF16),
            pltpu.VMEM((batch, model_dim), BF16),
            pltpu.VMEM((SLOTS, model_dim, TILE), BF16),
            pltpu.VMEM((RING, local_kv, CHUNK, head_dim), BF16),
            pltpu.VMEM((RING, local_kv, CHUNK, head_dim), BF16),
            pltpu.VMEM((batch, 8, head_dim), F32),
            pltpu.VMEM((local_kv, batch, head_dim), BF16),
            pltpu.VMEM((local_kv, batch, head_dim), BF16),
            pltpu.VMEM((batch, 8, lanes), F32),
            pltpu.VMEM((items, 8, lanes), F32),
            pltpu.VMEM((batch + 1, 8, lanes), F32),
            pltpu.VMEM((batch + 1, 8, lanes), F32),
            pltpu.VMEM((batch + 1, 8, head_dim), F32),
            pltpu.VMEM((batch, head_dim), F32),
            pltpu.VMEM((2, batch, head_dim), F32),
            pltpu.VMEM((model_dim,), BF16),
            pltpu.VMEM((1, head_dim), F32),
            pltpu.VMEM((batch, q_dim), BF16),
            pltpu.VMEM((batch, 2 * local_kv * head_dim), BF16),
            pltpu.VMEM((batch, width), BF16),
            pltpu.SMEM((items,), jnp.int32),
            pltpu.SMEM((items,), jnp.int32),
            dma((3,)), dma((3,)), dma((SLOTS,)), dma((RING // UNROLL,)), dma((RING // UNROLL,)),
        ],
        compiler_params=pltpu.CompilerParams(vmem_limit_bytes=VMEM_BYTES),
        name="front",
    )(lengths, tokens, norm_gain, freq, k_cache, v_cache, w_query, w_key, w_value, w_gate, w_up)


def back_kernel(hidden, tokens, attended, kv_new, w_down, w_out,
                y_out, key_out, value_out,
                u_buf, o_buf, kv_buf, x_buf, w_buf, wo_buf, part, from_sib, to_cross, from_cross, y_buf, kv_in, head_buf,
                in_sem, w_sem, wo_sem, kv_send, kv_recv, s1_send, s1_recv, s2_send, s2_recv,
                yc_send, yc_recv, ys_send, ys_recv, yr_send, yr_recv):
    me = lax.axis_index('model')
    core = lax.rem(me, 2)
    chip = lax.div(me, 2)
    sib = chip * 2 + (1 - core)
    cross = (1 - chip) * 2 + core
    diag = (1 - chip) * 2 + (1 - core)
    n_out = w_down.shape[1] // TILE
    head_dim = head_buf.shape[2]
    local_kv = kv_buf.shape[2] // (2 * head_dim)
    lag_sib, lag_cross, lag_relay, lag_store = LAGS

    barrier = pltpu.get_barrier_semaphore()
    for peer in (sib, cross, diag):
        pl.semaphore_signal(barrier, inc=1, device_id={'model': peer}, device_id_type=MESH)

    def cols(tile):
        return pl.ds(pl.multiple_of(tile * TILE, TILE), TILE)

    def down_copy(c):
        return pltpu.make_async_copy(w_down.at[:, cols(c)], w_buf.at[c], w_sem.at[c])

    def remote(src, dst, send, recv, peer):
        return pltpu.make_async_remote_copy(src_ref=src, dst_ref=dst, send_sem=send, recv_sem=recv,
                                            device_id={'model': peer}, device_id_type=MESH)

    def out_copy(c):
        return pltpu.make_async_copy(w_out.at[:, cols(c)], wo_buf.at[c], wo_sem.at[c])

    in_copies = [pltpu.make_async_copy(src, dst, in_sem.at[n]) for n, (src, dst) in
                 enumerate(((attended, o_buf), (hidden, u_buf), (kv_new, kv_buf), (tokens.at[me], x_buf)))]
    for copy in in_copies[:2]:
        copy.start()
    out_copy(0).start()
    down_copy(0).start()
    for copy in in_copies[2:]:
        copy.start()

    @pl.loop(1, n_out)
    def _(c):
        out_copy(c).start()
        down_copy(c).start()

    in_copies[2].wait()
    pl.semaphore_wait(barrier, 3)
    kv_sends = []
    for n, peer in enumerate((sib, cross, diag)):
        send = remote(kv_buf.at[peer], kv_in.at[me], kv_send.at[n], kv_recv.at[n], peer)
        send.start()
        kv_sends.append(send)
    for copy in (in_copies[0], in_copies[1], in_copies[3]):
        copy.wait()

    def sib_send(c):
        return remote(part.at[c, :, 1 - core], from_sib.at[c], s1_send.at[c], s1_recv.at[c], sib)

    def cross_send(c):
        return remote(to_cross.at[c], from_cross.at[c], s2_send.at[c], s2_recv.at[c], cross)

    def y_cross(c):
        return remote(y_buf.at[c, me], y_buf.at[c, me], yc_send.at[c], yc_recv.at[c], cross)

    def y_sib(c):
        return remote(y_buf.at[c, me], y_buf.at[c, me], ys_send.at[c], ys_recv.at[c], sib)

    def y_relay(c):
        return remote(y_buf.at[c, cross], y_buf.at[c, cross], yr_send.at[c], yr_recv.at[c], sib)

    @pl.loop(0, n_out + lag_store)
    def _(i):
        @pl.when(i < n_out)
        def _():
            out_copy(i).wait()
            total = jnp.dot(o_buf[...], wo_buf[i], preferred_element_type=F32)
            down_copy(i).wait()
            total += jnp.dot(u_buf[...], w_buf[i], preferred_element_type=F32)
            part[i] = total.reshape(part.shape[1:])
            sib_send(i).start()

        @pl.when((i >= lag_sib) & (i < n_out + lag_sib))
        def _():
            c = i - lag_sib
            sib_send(c).wait_recv()
            to_cross[c] = part[c, 1 - chip, core] + from_sib[c, 1 - chip]
            cross_send(c).start()

        @pl.when((i >= lag_cross) & (i < n_out + lag_cross))
        def _():
            c = i - lag_cross
            cross_send(c).wait_recv()
            total = part[c, chip, core] + from_sib[c, chip] + from_cross[c]
            y_buf[c, me] = (x_buf[:, cols(c)].astype(F32) + total).astype(BF16)
            y_cross(c).start()
            y_sib(c).start()

        @pl.when((i >= lag_relay) & (i < n_out + lag_relay))
        def _():
            c = i - lag_relay
            y_cross(c).wait_recv()
            y_relay(c).start()

        @pl.when(i == n_out)
        def _():
            for send in kv_sends:
                send.wait_recv()
            kv_in[me] = kv_buf[me]
            for half, out in enumerate((key_out, value_out)):
                for source in range(kv_in.shape[0]):
                    for g in range(local_kv):
                        start = (half * local_kv + g) * head_dim
                        head_buf[:, source * local_kv + g, :] = kv_in[source, :, start:start + head_dim].astype(F32)
                out[...] = head_buf[...].astype(BF16)

        @pl.when(i >= lag_store)
        def _():
            c = i - lag_store
            y_sib(c).wait_recv()
            y_relay(c).wait_recv()
            y_out[:, :, cols(c)] = y_buf[c]

    for send in kv_sends:
        send.wait_send()

    @pl.loop(0, n_out)
    def _(c):
        sib_send(c).wait_send()
        cross_send(c).wait_send()
        y_cross(c).wait_send()
        y_sib(c).wait_send()
        y_relay(c).wait_send()


def back(hidden, tokens, attended, kv_new, w_down, w_out, kv_heads, head_dim):
    batch, model_dim = tokens.shape
    width = w_down.shape[0]
    q_dim = w_out.shape[0]
    devices = 4
    rows = batch // devices
    n_out = model_dim // TILE
    kv_width = kv_new.shape[1]
    vmem = pl.BlockSpec(memory_space=pltpu.VMEM)
    dma = pltpu.SemaphoreType.DMA
    hbm = pl.BlockSpec(memory_space=pltpu.HBM)
    y, key_out, value_out = pl.pallas_call(
        back_kernel,
        out_shape=(jax.ShapeDtypeStruct((devices, rows, model_dim), BF16),
                   jax.ShapeDtypeStruct((rows, kv_heads, head_dim), BF16),
                   jax.ShapeDtypeStruct((rows, kv_heads, head_dim), BF16)),
        in_specs=[hbm] * 6,
        out_specs=(vmem, vmem, vmem),
        scratch_shapes=[
            pltpu.VMEM((batch, width), BF16),
            pltpu.VMEM((batch, q_dim), BF16),
            pltpu.VMEM((devices, rows, kv_width), BF16),
            pltpu.VMEM((rows, model_dim), BF16),
            pltpu.VMEM((n_out, width, TILE), BF16),
            pltpu.VMEM((n_out, q_dim, TILE), BF16),
            pltpu.VMEM((n_out, 2, 2, rows, TILE), F32),
            pltpu.VMEM((n_out, 2, rows, TILE), F32),
            pltpu.VMEM((n_out, rows, TILE), F32),
            pltpu.VMEM((n_out, rows, TILE), F32),
            pltpu.VMEM((n_out, devices, rows, TILE), BF16),
            pltpu.VMEM((devices, rows, kv_width), BF16),
            pltpu.VMEM((rows, kv_heads, head_dim), F32),
            dma((4,)), dma((n_out,)), dma((n_out,)), dma((3,)), dma((3,)),
        ] + [dma((n_out,))] * 10,
        compiler_params=pltpu.CompilerParams(collective_id=0, has_side_effects=True, vmem_limit_bytes=VMEM_BYTES - RESULT_BYTES),
        name="back",
    )(hidden, tokens.reshape(devices, rows, model_dim), attended, kv_new.reshape(devices, rows, kv_width), w_down, w_out)
    return finish(y.reshape(batch, model_dim), key_out, value_out)


def finish_kernel(*refs):
    half = (len(refs) - 1) // 2
    copies = [pltpu.make_async_copy(refs[n], refs[half + n], refs[-1].at[n]) for n in range(half)]
    for copy in copies:
        copy.start()
    for copy in copies:
        copy.wait()


def finish(*arrays):
    return pl.pallas_call(
        finish_kernel,
        out_shape=tuple(jax.ShapeDtypeStruct(a.shape, a.dtype) for a in arrays),
        in_specs=[pl.BlockSpec(memory_space=pltpu.VMEM)] * len(arrays),
        out_specs=tuple(pl.BlockSpec(memory_space=pltpu.HBM) for _ in arrays),
        scratch_shapes=[pltpu.SemaphoreType.DMA((len(arrays),))],
        compiler_params=pltpu.CompilerParams(vmem_limit_bytes=4 * 2 ** 20),
        name="finish",
    )(*arrays)


def solution(mesh):
    groups = mesh.shape['model']

    def local_step(tokens, lengths, k_cache, v_cache, norm_gain, w_query, w_key, w_value, w_out, w_gate, w_up, w_down):
        kv_heads, _, head_dim = k_cache.shape[1:]
        attended, kv_new, hidden = front(tokens, lengths, k_cache, v_cache, norm_gain, w_query, w_key, w_value, w_gate, w_up, groups)
        return back(hidden, tokens, attended, kv_new, w_down, w_out, kv_heads, head_dim)

    in_specs = (P('replica', None), P('replica'), P('replica', None, None, None), P('replica', None, None, None), P(None), P(None, 'model'), P(None, None), P(None, None), P('model', None), P(None, 'model'), P(None, 'model'), P('model', None))
    out_specs = (P('replica', None), P(('replica', 'model'), None, None), P(('replica', 'model'), None, None))
    return jax.shard_map(local_step, mesh=mesh, in_specs=in_specs, out_specs=out_specs, check_vma=False)
```

```python
import functools
import math

import jax
import jax.numpy as jnp
import numpy as np
from jax import lax
from jax.experimental import pallas as pl
from jax.experimental.pallas import tpu as pltpu
from jax.sharding import PartitionSpec as P

ROPE_BASE = 10000.0
NORM_EPS = 1e-6
MASK_VALUE = -1e30
MESH = pl.DeviceIdType.MESH
F32 = jnp.float32
BF16 = jnp.bfloat16
TILE = 256
SLOTS = 12
LAGS = (1, 6, 11, 13)
CHUNK = 64
UNROLL = 16
VMEM_BYTES = 67_043_328
RESULT_BYTES = 12_000_000
PIECES_SCORE = 12
PIECES_VALUE = 11
RING = 256


def front_kernel(lengths, tokens, gain_hbm, freq_hbm, k_cache, v_cache, w_query, w_key, w_value, w_gate, w_up,
                 packed,
                 x_buf, h_buf, w_buf, k_ring, v_ring, q_buf, kn_buf, vn_buf, fresh, score, peak, total, mixed, angle, rot,
                 gain, freq, o_out, kv_out, u_out,
                 item_seq, item_pos, out_sem, x_sem, w_sem, k_sem, v_sem):
    batch, model_dim = tokens.shape
    head_dim = freq.shape[1]
    local_kv = kv_out.shape[1] // (2 * head_dim)
    heads = o_out.shape[1] // head_dim
    ratio = heads // local_kv
    q_tiles = w_query.shape[1] // TILE
    lead = q_tiles + 2
    half = TILE // 2
    pieces = w_gate.shape[1] // half
    ring_steps = RING // UNROLL
    first_steps = batch // UNROLL
    scale = head_dim ** -0.5
    me = lax.axis_index('model')
    local = pl.ds(me * local_kv, local_kv)
    lanes = local_kv * CHUNK

    def w_copy(src, tile, t):
        return pltpu.make_async_copy(src.at[:, pl.ds(pl.multiple_of(tile * TILE, TILE), TILE)], w_buf.at[t], w_sem.at[t])

    def start_piece(p, slot):
        for n, src in enumerate((w_gate, w_up)):
            pltpu.make_async_copy(src.at[:, pl.ds(pl.multiple_of(p * half, half), half)],
                                  w_buf.at[slot, :, n * half:(n + 1) * half], w_sem.at[slot]).start()

    def first_copy(cache, ring, sem, step):
        rows = pl.ds(step * UNROLL, UNROLL)
        return pltpu.make_async_copy(cache.at[rows, local, pl.ds(0, CHUNK)], ring.at[rows], sem.at[step])

    def item_copy(cache, ring, sem, k):
        slot = lax.rem(k, RING)
        return pltpu.make_async_copy(cache.at[lax.rem(item_seq[k], batch), local, pl.ds(pl.multiple_of(item_pos[k], CHUNK), CHUNK)],
                                     ring.at[slot], sem.at[lax.div(slot, UNROLL)])

    x_copy = pltpu.make_async_copy(tokens, x_buf, x_sem.at[0])
    gain_copy = pltpu.make_async_copy(gain_hbm, gain, x_sem.at[1])
    freq_copy = pltpu.make_async_copy(freq_hbm, freq, x_sem.at[2])
    for copy in (freq_copy, x_copy, gain_copy):
        copy.start()
    lead_copies = [w_copy(w_key, me, 0), w_copy(w_value, me, 1)] + [w_copy(w_query, t, 2 + t) for t in range(q_tiles)]
    for copy in lead_copies:
        copy.start()
    for step in range(first_steps):
        first_copy(k_cache, k_ring, k_sem, step).start()
    for p in range(SLOTS - lead):
        start_piece(p, lead + p)
    for step in range(first_steps):
        first_copy(v_cache, v_ring, v_sem, step).start()

    def second(i, k):
        for r in range(UNROLL):
            seq = i * UNROLL + r
            item_seq[k] = seq
            item_pos[k] = CHUNK
            k = k + (lengths[seq] > CHUNK).astype(jnp.int32)
        return k

    begin = batch
    end = lax.fori_loop(0, batch // UNROLL, second, batch)
    for c in range(2, k_cache.shape[2] // CHUNK):
        def further(i, k):
            seq = item_seq[i]
            item_seq[k] = seq
            item_pos[k] = c * CHUNK
            return k + (lengths[seq] > c * CHUNK).astype(jnp.int32)

        begin, end = end, lax.fori_loop(begin, end, further, end)
    steps = lax.div(end + (UNROLL - 1), UNROLL)

    @pl.loop(end, steps * UNROLL)
    def _(k):
        item_seq[k] = batch
        item_pos[k] = 0

    @pl.loop(batch, jnp.minimum(steps * UNROLL, RING))
    def _(k):
        item_copy(k_cache, k_ring, k_sem, k).start()
        item_copy(v_cache, v_ring, v_sem, k).start()

    freq_copy.wait()

    @pl.loop(0, batch // 8)
    def _(i):
        for r in range(8):
            angle[pl.ds(i * 8 + r, 1), :] = lengths[i * 8 + r].astype(F32) * freq[...]

    first = lax.broadcasted_iota(jnp.int32, (batch, head_dim), 1) < head_dim // 2
    rot[0] = jnp.cos(angle[...])
    rot[1] = jnp.where(first, -jnp.sin(angle[...]), jnp.sin(angle[...]))
    q_buf[...] = jnp.zeros(q_buf.shape, F32)

    x_copy.wait()
    gain_copy.wait()
    x = x_buf[...].astype(F32)
    mean_sq = jnp.mean(x * x, axis=-1, keepdims=True)
    h_buf[...] = (x * lax.rsqrt(mean_sq + NORM_EPS) * gain[...].reshape(1, model_dim).astype(F32)).astype(BF16)

    def rope(a):
        return a * rot[0] + pltpu.roll(a, head_dim // 2, 1) * rot[1]

    for t, copy in enumerate(lead_copies):
        copy.wait()
        prod = jnp.dot(h_buf[...], w_buf[t], preferred_element_type=F32)
        if SLOTS - lead + t < pieces:
            start_piece(SLOTS - lead + t, t)
        for j in range(TILE // head_dim):
            a = prod[:, j * head_dim:(j + 1) * head_dim]
            if t >= 2:
                q_buf[:, (t - 2) * (TILE // head_dim) + j, :] = rope(a).astype(BF16).astype(F32)
            else:
                a = (rope(a) if t == 0 else a).astype(BF16)
                col = (t * local_kv + j) * head_dim
                kv_out[:, col:col + head_dim] = a
                (kn_buf, vn_buf)[t][j] = a
    width = u_out.shape[1]
    o_at, kv_at = width, width + heads * head_dim
    x_at = kv_at + kv_out.shape[1]
    kv_copy = pltpu.make_async_copy(kv_out, packed.at[:, kv_at:x_at], out_sem.at[0])
    kv_copy.start()
    quarter = batch // 4
    x_part = model_dim // 4
    x_rows = pl.ds(pl.multiple_of(me * quarter, quarter), quarter)
    x_copies = [pltpu.make_async_copy(x_buf.at[x_rows, n * x_part:(n + 1) * x_part],
                                      packed.at[n * quarter:(n + 1) * quarter, x_at:x_at + x_part], out_sem.at[3 + n]) for n in range(4)]
    for copy in x_copies:
        copy.start()
    peak[batch] = jnp.full(peak.shape[1:], MASK_VALUE, F32)
    total[batch] = jnp.zeros(total.shape[1:], F32)
    mixed[batch] = jnp.zeros(mixed.shape[1:], F32)

    sub = q_buf.shape[1]
    lane = lax.broadcasted_iota(jnp.int32, (sub, lanes), 1)
    head = lax.broadcasted_iota(jnp.int32, (sub, lanes), 0)
    own = (lax.div(lane, CHUNK) == lax.div(head, ratio)) & (head < heads)
    pos_in = jnp.where(own, lax.rem(lane, CHUNK), 1 << 20)

    line = lax.broadcasted_iota(jnp.int32, (CHUNK, sub, lanes), 0)
    mine = line == pos_in[None]
    blocks = [slice(b0, b0 + CHUNK) for b0 in range(0, batch, CHUNK)]
    for rows in blocks:
        q = q_buf[rows].reshape(CHUNK * sub, head_dim).astype(BF16)
        s = lax.dot_general(q, kn_buf[:, rows].reshape(lanes, head_dim), (((1,), (1,)), ((), ())), preferred_element_type=F32) * scale
        s = jnp.where(mine, s.reshape(CHUNK, sub, lanes), MASK_VALUE)
        fresh[rows] = s
        peak[rows] = s

    def wait_step(ring, sem, step):
        at = lax.rem(step, ring_steps)
        pltpu.make_async_copy(ring.at[pl.ds(0, UNROLL)], ring.at[pl.ds(at * UNROLL, UNROLL)], sem.at[at]).wait()

    def refill(cache, ring, sem, step):
        @pl.when(step + ring_steps < steps)
        def _():
            @pl.loop(0, UNROLL)
            def _(u):
                item_copy(cache, ring, sem, (step + ring_steps) * UNROLL + u).start()

    def item(step, u, listed):
        k = step * UNROLL + u
        if listed:
            return k, item_seq[k], lax.rem(item_seq[k], batch), item_pos[k]
        return k, k, k, 0

    def score_step(step, listed):
        base = lax.rem(step, ring_steps) * UNROLL
        found = []
        for u in range(UNROLL):
            k, seq, row, pos = item(step, u, listed)
            keys = k_ring[base + u].reshape(lanes, head_dim)
            s = lax.dot_general(q_buf[row].astype(BF16), keys, (((1,), (1,)), ((), ())), preferred_element_type=F32) * scale
            s = jnp.where(pos_in < lengths[row] - pos, s, MASK_VALUE)
            score[k] = s
            found.append((seq, s))
        for seq, s in found:
            peak[seq] = jnp.maximum(peak[seq], s)

    def value_step(step, listed):
        base = lax.rem(step, ring_steps) * UNROLL
        found = []
        for u in range(UNROLL):
            k, seq, row, pos = item(step, u, listed)
            p = jnp.exp(score[k] - peak[seq])
            values = v_ring[base + u].reshape(lanes, head_dim)
            found.append((seq, p, jnp.dot(p.astype(BF16), values, preferred_element_type=F32)))
        for seq, p, o in found:
            total[seq] = total[seq] + p
            mixed[seq] = mixed[seq] + o

    def u_copy(p):
        cols = pl.ds(pl.multiple_of(p * half, half), half)
        return pltpu.make_async_copy(u_out.at[:, cols], packed.at[:, cols], out_sem.at[1])

    def wait_piece(p):
        slot = lax.rem(lead + p, SLOTS)
        pltpu.make_async_copy(w_gate.at[:, pl.ds(0, TILE)], w_buf.at[slot], w_sem.at[slot]).wait()

    def piece(p):
        prod = jnp.dot(h_buf[...], w_buf[lax.rem(lead + p, SLOTS)], preferred_element_type=F32)
        u_out[:, pl.ds(pl.multiple_of(p * half, half), half)] = (jax.nn.silu(prod[:, :half]) * prod[:, half:]).astype(BF16)

    def after_piece(p):
        u_copy(p).start()

        @pl.when(p + SLOTS < pieces)
        def _():
            start_piece(p + SLOTS, lax.rem(lead + p, SLOTS))

    def both(attend_step, cache, ring, sem, p0, p1):
        @pl.loop(0, first_steps)
        def _(s):
            wait_step(ring, sem, s)
            wait_piece(p0 + s)
            attend_step(s, False)
            piece(p0 + s)
            refill(cache, ring, sem, s)
            after_piece(p0 + s)

        fused = jnp.minimum(steps, p1 - p0)

        @pl.loop(first_steps, fused)
        def _(s):
            wait_step(ring, sem, s)
            wait_piece(p0 + s)
            attend_step(s, True)
            piece(p0 + s)
            refill(cache, ring, sem, s)
            after_piece(p0 + s)

        @pl.loop(fused, steps)
        def _(s):
            wait_step(ring, sem, s)
            attend_step(s, True)
            refill(cache, ring, sem, s)

        return p0 + fused

    reached = both(score_step, k_cache, k_ring, k_sem, 0, PIECES_SCORE)

    @pl.loop(reached, PIECES_SCORE)
    def _(p):
        wait_piece(p)
        piece(p)
        after_piece(p)

    for rows in blocks:
        top = jnp.broadcast_to(jnp.max(peak[rows], axis=-1, keepdims=True), (CHUNK, sub, lanes))
        peak[rows] = top
        p = jnp.exp(fresh[rows] - top)
        total[rows] = p
        o = jnp.dot(p.reshape(CHUNK * sub, lanes).astype(BF16), vn_buf[:, rows].reshape(lanes, head_dim), preferred_element_type=F32)
        mixed[rows] = o.reshape(CHUNK, sub, head_dim)

    reached = both(value_step, v_cache, v_ring, v_sem, PIECES_SCORE, PIECES_SCORE + PIECES_VALUE)

    q_buf[...] = mixed[:batch] / jnp.sum(total[:batch], axis=-1, keepdims=True)
    for h in range(heads):
        o_out[:, h * head_dim:(h + 1) * head_dim] = q_buf[:, h, :].astype(BF16)
    o_copy = pltpu.make_async_copy(o_out, packed.at[:, o_at:kv_at], out_sem.at[2])
    o_copy.start()

    @pl.loop(reached, pieces)
    def _(p):
        wait_piece(p)
        piece(p)
        after_piece(p)

    kv_copy.wait()
    o_copy.wait()
    for copy in x_copies:
        copy.wait()
    pltpu.make_async_copy(u_out, packed.at[:, :width], out_sem.at[1]).wait()


def front(tokens, lengths, k_cache, v_cache, norm_gain, w_query, w_key, w_value, w_gate, w_up, groups):
    batch, model_dim = tokens.shape
    kv_heads, context, head_dim = k_cache.shape[1:]
    local_kv = kv_heads // groups
    q_dim = w_query.shape[1]
    width = w_gate.shape[1]
    half_freq = np.exp(np.arange(head_dim // 2) * (-2.0 * math.log(ROPE_BASE) / head_dim))
    freq = jnp.asarray(np.concatenate([half_freq, half_freq])[None, :], F32)
    items = batch * (context // CHUNK) + UNROLL
    lanes = local_kv * CHUNK
    dma = pltpu.SemaphoreType.DMA
    hbm = pl.BlockSpec(memory_space=pltpu.HBM)
    smem = pl.BlockSpec(memory_space=pltpu.SMEM)
    return pl.pallas_call(
        front_kernel,
        out_shape=jax.ShapeDtypeStruct((batch, width + q_dim + 2 * local_kv * head_dim + model_dim // 4), BF16),
        in_specs=[smem] + [hbm] * 10,
        out_specs=hbm,
        scratch_shapes=[
            pltpu.VMEM((batch, model_dim), BF16),
            pltpu.VMEM((batch, model_dim), BF16),
            pltpu.VMEM((SLOTS, model_dim, TILE), BF16),
            pltpu.VMEM((RING, local_kv, CHUNK, head_dim), BF16),
            pltpu.VMEM((RING, local_kv, CHUNK, head_dim), BF16),
            pltpu.VMEM((batch, 8, head_dim), F32),
            pltpu.VMEM((local_kv, batch, head_dim), BF16),
            pltpu.VMEM((local_kv, batch, head_dim), BF16),
            pltpu.VMEM((batch, 8, lanes), F32),
            pltpu.VMEM((items, 8, lanes), F32),
            pltpu.VMEM((batch + 1, 8, lanes), F32),
            pltpu.VMEM((batch + 1, 8, lanes), F32),
            pltpu.VMEM((batch + 1, 8, head_dim), F32),
            pltpu.VMEM((batch, head_dim), F32),
            pltpu.VMEM((2, batch, head_dim), F32),
            pltpu.VMEM((model_dim,), BF16),
            pltpu.VMEM((1, head_dim), F32),
            pltpu.VMEM((batch, q_dim), BF16),
            pltpu.VMEM((batch, 2 * local_kv * head_dim), BF16),
            pltpu.VMEM((batch, width), BF16),
            pltpu.SMEM((items,), jnp.int32),
            pltpu.SMEM((items,), jnp.int32),
            dma((7,)), dma((3,)), dma((SLOTS,)), dma((RING // UNROLL,)), dma((RING // UNROLL,)),
        ],
        compiler_params=pltpu.CompilerParams(vmem_limit_bytes=VMEM_BYTES),
        name="front",
    )(lengths, tokens, norm_gain, freq, k_cache, v_cache, w_query, w_key, w_value, w_gate, w_up)


def back_kernel(packed, w_down, w_out,
                y_out, key_out, value_out, _,
                u_buf, o_buf, kv_buf, x_buf, w_buf, wo_buf, part, from_sib, to_cross, from_cross, y_buf, kv_in, head_buf,
                in_sem, w_sem, wo_sem, kv_send, kv_recv, s1_send, s1_recv, s2_send, s2_recv,
                yc_send, yc_recv, ys_send, ys_recv, yr_send, yr_recv):
    me = lax.axis_index('model')
    core = lax.rem(me, 2)
    chip = lax.div(me, 2)
    sib = chip * 2 + (1 - core)
    cross = (1 - chip) * 2 + core
    diag = (1 - chip) * 2 + (1 - core)
    n_out = w_down.shape[1] // TILE
    head_dim = head_buf.shape[2]
    local_kv = kv_buf.shape[2] // (2 * head_dim)
    lag_sib, lag_cross, lag_relay, lag_store = LAGS

    barrier = pltpu.get_barrier_semaphore()
    for peer in (sib, cross, diag):
        pl.semaphore_signal(barrier, inc=1, device_id={'model': peer}, device_id_type=MESH)

    def cols(tile):
        return pl.ds(pl.multiple_of(tile * TILE, TILE), TILE)

    def down_copy(c):
        return pltpu.make_async_copy(w_down.at[:, cols(c)], w_buf.at[c], w_sem.at[c])

    def remote(src, dst, send, recv, peer):
        return pltpu.make_async_remote_copy(src_ref=src, dst_ref=dst, send_sem=send, recv_sem=recv,
                                            device_id={'model': peer}, device_id_type=MESH)

    def out_copy(c):
        return pltpu.make_async_copy(w_out.at[:, cols(c)], wo_buf.at[c], wo_sem.at[c])

    devices, rows = kv_buf.shape[:2]
    width, q_dim = u_buf.shape[1], o_buf.shape[1]
    kv_at = width + q_dim
    x_at = kv_at + kv_buf.shape[2]
    x_part = x_buf.shape[2]
    o_copy = pltpu.make_async_copy(packed.at[:, width:kv_at], o_buf, in_sem.at[0])
    u_copy = pltpu.make_async_copy(packed.at[:, :width], u_buf, in_sem.at[1])
    kv_copies = [pltpu.make_async_copy(packed.at[n * rows:(n + 1) * rows, kv_at:x_at], kv_buf.at[n], in_sem.at[2 + n]) for n in range(devices)]
    x_copies = [pltpu.make_async_copy(packed.at[n * rows:(n + 1) * rows, x_at:x_at + x_part], x_buf.at[n], in_sem.at[2 + devices + n])
                for n in range(devices)]
    for copy in (o_copy, u_copy, out_copy(0), down_copy(0), *kv_copies, *x_copies):
        copy.start()

    @pl.loop(1, n_out)
    def _(c):
        out_copy(c).start()
        down_copy(c).start()

    for copy in kv_copies:
        copy.wait()
    pl.semaphore_wait(barrier, 3)
    kv_sends = []
    for n, peer in enumerate((sib, cross, diag)):
        send = remote(kv_buf.at[peer], kv_in.at[me], kv_send.at[n], kv_recv.at[n], peer)
        send.start()
        kv_sends.append(send)
    for copy in (o_copy, u_copy, *x_copies):
        copy.wait()

    def sib_send(c):
        return remote(part.at[c, :, 1 - core], from_sib.at[c], s1_send.at[c], s1_recv.at[c], sib)

    def cross_send(c):
        return remote(to_cross.at[c], from_cross.at[c], s2_send.at[c], s2_recv.at[c], cross)

    def y_cross(c):
        return remote(y_buf.at[c, me], y_buf.at[c, me], yc_send.at[c], yc_recv.at[c], cross)

    def y_sib(c):
        return remote(y_buf.at[c, me], y_buf.at[c, me], ys_send.at[c], ys_recv.at[c], sib)

    def y_relay(c):
        return remote(y_buf.at[c, cross], y_buf.at[c, cross], yr_send.at[c], yr_recv.at[c], sib)

    @pl.loop(0, n_out + lag_store)
    def _(i):
        @pl.when(i < n_out)
        def _():
            out_copy(i).wait()
            total = jnp.dot(o_buf[...], wo_buf[i], preferred_element_type=F32)
            down_copy(i).wait()
            total += jnp.dot(u_buf[...], w_buf[i], preferred_element_type=F32)
            part[i] = total.reshape(part.shape[1:])
            sib_send(i).start()

        @pl.when((i >= lag_sib) & (i < n_out + lag_sib))
        def _():
            c = i - lag_sib
            sib_send(c).wait_recv()
            to_cross[c] = part[c, 1 - chip, core] + from_sib[c, 1 - chip]
            cross_send(c).start()

        @pl.when((i >= lag_cross) & (i < n_out + lag_cross))
        def _():
            c = i - lag_cross
            cross_send(c).wait_recv()
            total = part[c, chip, core] + from_sib[c, chip] + from_cross[c]
            x = x_buf[lax.div(c * TILE, x_part), :, pl.ds(pl.multiple_of(lax.rem(c * TILE, x_part), TILE), TILE)]
            y_buf[c, me] = (x.astype(F32) + total).astype(BF16)
            y_cross(c).start()
            y_sib(c).start()

        @pl.when((i >= lag_relay) & (i < n_out + lag_relay))
        def _():
            c = i - lag_relay
            y_cross(c).wait_recv()
            y_relay(c).start()

        @pl.when(i == n_out)
        def _():
            for send in kv_sends:
                send.wait_recv()
            kv_in[me] = kv_buf[me]
            for half, out in enumerate((key_out, value_out)):
                for source in range(kv_in.shape[0]):
                    for g in range(local_kv):
                        start = (half * local_kv + g) * head_dim
                        head_buf[:, source * local_kv + g, :] = kv_in[source, :, start:start + head_dim].astype(F32)
                out[...] = head_buf[...].astype(BF16)

        @pl.when(i >= lag_store)
        def _():
            c = i - lag_store
            y_sib(c).wait_recv()
            y_relay(c).wait_recv()
            y_out[:, :, cols(c)] = y_buf[c]

    for send in kv_sends:
        send.wait_send()

    @pl.loop(0, n_out)
    def _(c):
        sib_send(c).wait_send()
        cross_send(c).wait_send()
        y_cross(c).wait_send()
        y_sib(c).wait_send()
        y_relay(c).wait_send()


def back(packed, w_down, w_out, kv_heads, head_dim, devices):
    batch = packed.shape[0]
    width, model_dim = w_down.shape
    q_dim = w_out.shape[0]
    rows = batch // devices
    n_out = model_dim // TILE
    kv_width = 2 * (kv_heads // devices) * head_dim
    dma = pltpu.SemaphoreType.DMA
    hbm = pl.BlockSpec(memory_space=pltpu.HBM)
    vmem = pl.BlockSpec(memory_space=pltpu.VMEM)
    y, key_out, value_out, _ = pl.pallas_call(
        back_kernel,
        out_shape=(jax.ShapeDtypeStruct((devices, rows, model_dim), BF16),
                   jax.ShapeDtypeStruct((rows, kv_heads, head_dim), BF16),
                   jax.ShapeDtypeStruct((rows, kv_heads, head_dim), BF16),
                   jax.ShapeDtypeStruct(packed.shape, BF16)),
        in_specs=[hbm] * 3,
        out_specs=(vmem, vmem, vmem, hbm),
        input_output_aliases={0: 3},
        scratch_shapes=[
            pltpu.VMEM((batch, width), BF16),
            pltpu.VMEM((batch, q_dim), BF16),
            pltpu.VMEM((devices, rows, kv_width), BF16),
            pltpu.VMEM((4, rows, model_dim // 4), BF16),
            pltpu.VMEM((n_out, width, TILE), BF16),
            pltpu.VMEM((n_out, q_dim, TILE), BF16),
            pltpu.VMEM((n_out, 2, 2, rows, TILE), F32),
            pltpu.VMEM((n_out, 2, rows, TILE), F32),
            pltpu.VMEM((n_out, rows, TILE), F32),
            pltpu.VMEM((n_out, rows, TILE), F32),
            pltpu.VMEM((n_out, devices, rows, TILE), BF16),
            pltpu.VMEM((devices, rows, kv_width), BF16),
            pltpu.VMEM((rows, kv_heads, head_dim), F32),
            dma((2 + 2 * devices,)), dma((n_out,)), dma((n_out,)), dma((3,)), dma((3,)),
        ] + [dma((n_out,))] * 10,
        compiler_params=pltpu.CompilerParams(collective_id=0, has_side_effects=True, vmem_limit_bytes=VMEM_BYTES - RESULT_BYTES),
        name="back",
    )(packed, w_down, w_out)
    return finish(y.reshape(batch, model_dim), key_out, value_out)


def finish_kernel(*refs):
    half = (len(refs) - 1) // 2
    copies = [pltpu.make_async_copy(refs[n], refs[half + n], refs[-1].at[n]) for n in range(half)]
    for copy in copies:
        copy.start()
    for copy in copies:
        copy.wait()


def finish(*arrays):
    return pl.pallas_call(
        finish_kernel,
        out_shape=tuple(jax.ShapeDtypeStruct(a.shape, a.dtype) for a in arrays),
        in_specs=[pl.BlockSpec(memory_space=pltpu.VMEM)] * len(arrays),
        out_specs=tuple(pl.BlockSpec(memory_space=pltpu.HBM) for _ in arrays),
        scratch_shapes=[pltpu.SemaphoreType.DMA((len(arrays),))],
        compiler_params=pltpu.CompilerParams(vmem_limit_bytes=4 * 2 ** 20),
        name="finish",
    )(*arrays)


def solution(mesh):
    groups = mesh.shape['model']

    def local_step(tokens, lengths, k_cache, v_cache, norm_gain, w_query, w_key, w_value, w_out, w_gate, w_up, w_down):
        kv_heads, _, head_dim = k_cache.shape[1:]
        packed = front(tokens, lengths, k_cache, v_cache, norm_gain, w_query, w_key, w_value, w_gate, w_up, groups)
        return back(packed, w_down, w_out, kv_heads, head_dim, groups)

    in_specs = (P('replica', None), P('replica'), P('replica', None, None, None), P('replica', None, None, None), P(None), P(None, 'model'), P(None, None), P(None, None), P('model', None), P(None, 'model'), P(None, 'model'), P('model', None))
    out_specs = (P('replica', None), P(('replica', 'model'), None, None), P(('replica', 'model'), None, None))
    return jax.shard_map(local_step, mesh=mesh, in_specs=in_specs, out_specs=out_specs, check_vma=False)
```

```python
import functools
import math

import jax
import jax.numpy as jnp
import numpy as np
from jax import lax
from jax.experimental import pallas as pl
from jax.experimental.pallas import tpu as pltpu
from jax.sharding import PartitionSpec as P

ROPE_BASE = 10000.0
NORM_EPS = 1e-6
MASK_VALUE = -1e30
MESH = pl.DeviceIdType.MESH
F32 = jnp.float32
BF16 = jnp.bfloat16
TILE = 256
SLOTS = 12
LAGS = (1, 6, 11, 13)
CHUNK = 64
UNROLL = 16
VMEM_BYTES = 67_043_328
RESULT_BYTES = 12_000_000
PIECES_SCORE = 12
PIECES_VALUE = 11
RING = 256


def front_kernel(lengths, tokens, gain_hbm, freq_hbm, k_cache, v_cache, w_query, w_key, w_value, w_gate, w_up,
                 packed,
                 x_buf, h_buf, w_buf, k_ring, v_ring, q_buf, kn_buf, vn_buf, fresh, score, peak, total, mixed, angle, rot,
                 gain, freq, o_out, kv_out, u_out,
                 item_seq, item_pos, out_sem, x_sem, w_sem, k_sem, v_sem):
    batch, model_dim = tokens.shape
    head_dim = freq.shape[1]
    local_kv = kv_out.shape[1] // (2 * head_dim)
    heads = o_out.shape[1] // head_dim
    ratio = heads // local_kv
    q_tiles = w_query.shape[1] // TILE
    lead = q_tiles + 2
    half = TILE // 2
    pieces = w_gate.shape[1] // half
    ring_steps = RING // UNROLL
    first_steps = batch // UNROLL
    scale = head_dim ** -0.5
    me = lax.axis_index('model')
    local = pl.ds(me * local_kv, local_kv)
    lanes = local_kv * CHUNK

    def w_copy(src, tile, t):
        return pltpu.make_async_copy(src.at[:, pl.ds(pl.multiple_of(tile * TILE, TILE), TILE)], w_buf.at[t], w_sem.at[t])

    def start_piece(p, slot):
        for n, src in enumerate((w_gate, w_up)):
            pltpu.make_async_copy(src.at[:, pl.ds(pl.multiple_of(p * half, half), half)],
                                  w_buf.at[slot, :, n * half:(n + 1) * half], w_sem.at[slot]).start()

    def first_copy(cache, ring, sem, step):
        rows = pl.ds(step * UNROLL, UNROLL)
        return pltpu.make_async_copy(cache.at[rows, local, pl.ds(0, CHUNK)], ring.at[rows], sem.at[step])

    def item_copy(cache, ring, sem, k):
        slot = lax.rem(k, RING)
        return pltpu.make_async_copy(cache.at[lax.rem(item_seq[k], batch), local, pl.ds(pl.multiple_of(item_pos[k], CHUNK), CHUNK)],
                                     ring.at[slot], sem.at[lax.div(slot, UNROLL)])

    x_copy = pltpu.make_async_copy(tokens, x_buf, x_sem.at[0])
    gain_copy = pltpu.make_async_copy(gain_hbm, gain, x_sem.at[1])
    freq_copy = pltpu.make_async_copy(freq_hbm, freq, x_sem.at[2])
    for copy in (freq_copy, x_copy, gain_copy):
        copy.start()
    lead_copies = [w_copy(w_key, me, 0), w_copy(w_value, me, 1)] + [w_copy(w_query, t, 2 + t) for t in range(q_tiles)]
    for copy in lead_copies:
        copy.start()
    for step in range(first_steps):
        first_copy(k_cache, k_ring, k_sem, step).start()
    for p in range(SLOTS - lead):
        start_piece(p, lead + p)
    for step in range(first_steps):
        first_copy(v_cache, v_ring, v_sem, step).start()

    def second(i, k):
        for r in range(UNROLL):
            seq = i * UNROLL + r
            item_seq[k] = seq
            item_pos[k] = CHUNK
            k = k + (lengths[seq] > CHUNK).astype(jnp.int32)
        return k

    begin = batch
    end = lax.fori_loop(0, batch // UNROLL, second, batch)
    for c in range(2, k_cache.shape[2] // CHUNK):
        def further(i, k):
            seq = item_seq[i]
            item_seq[k] = seq
            item_pos[k] = c * CHUNK
            return k + (lengths[seq] > c * CHUNK).astype(jnp.int32)

        begin, end = end, lax.fori_loop(begin, end, further, end)
    steps = lax.div(end + (UNROLL - 1), UNROLL)

    @pl.loop(end, steps * UNROLL)
    def _(k):
        item_seq[k] = batch
        item_pos[k] = 0

    @pl.loop(batch, jnp.minimum(steps * UNROLL, RING))
    def _(k):
        item_copy(k_cache, k_ring, k_sem, k).start()
        item_copy(v_cache, v_ring, v_sem, k).start()

    freq_copy.wait()

    @pl.loop(0, batch // 8)
    def _(i):
        for r in range(8):
            angle[pl.ds(i * 8 + r, 1), :] = lengths[i * 8 + r].astype(F32) * freq[...]

    first = lax.broadcasted_iota(jnp.int32, (batch, head_dim), 1) < head_dim // 2
    rot[0] = jnp.cos(angle[...])
    rot[1] = jnp.where(first, -jnp.sin(angle[...]), jnp.sin(angle[...]))
    q_buf[...] = jnp.zeros(q_buf.shape, F32)

    x_copy.wait()
    gain_copy.wait()
    x = x_buf[...].astype(F32)
    mean_sq = jnp.mean(x * x, axis=-1, keepdims=True)
    h_buf[...] = (x * lax.rsqrt(mean_sq + NORM_EPS) * gain[...].reshape(1, model_dim).astype(F32)).astype(BF16)

    def rope(a):
        return a * rot[0] + pltpu.roll(a, head_dim // 2, 1) * rot[1]

    for t, copy in enumerate(lead_copies):
        copy.wait()
        prod = jnp.dot(h_buf[...], w_buf[t], preferred_element_type=F32)
        if SLOTS - lead + t < pieces:
            start_piece(SLOTS - lead + t, t)
        for j in range(TILE // head_dim):
            a = prod[:, j * head_dim:(j + 1) * head_dim]
            if t >= 2:
                q_buf[:, (t - 2) * (TILE // head_dim) + j, :] = rope(a).astype(BF16).astype(F32)
            else:
                a = (rope(a) if t == 0 else a).astype(BF16)
                col = (t * local_kv + j) * head_dim
                kv_out[:, col:col + head_dim] = a
                (kn_buf, vn_buf)[t][j] = a
    width = u_out.shape[1]
    o_at, kv_at = width, width + heads * head_dim
    x_at = kv_at + kv_out.shape[1]
    kv_copy = pltpu.make_async_copy(kv_out, packed.at[:, kv_at:x_at], out_sem.at[0])
    kv_copy.start()
    quarter = batch // 4
    x_part = model_dim // 4
    x_rows = pl.ds(pl.multiple_of(me * quarter, quarter), quarter)
    x_copies = [pltpu.make_async_copy(x_buf.at[x_rows, n * x_part:(n + 1) * x_part],
                                      packed.at[n * quarter:(n + 1) * quarter, x_at:x_at + x_part], out_sem.at[3 + n]) for n in range(4)]
    for copy in x_copies:
        copy.start()
    peak[batch] = jnp.full(peak.shape[1:], MASK_VALUE, F32)
    total[batch] = jnp.zeros(total.shape[1:], F32)
    mixed[batch] = jnp.zeros(mixed.shape[1:], F32)

    sub = q_buf.shape[1]
    lane = lax.broadcasted_iota(jnp.int32, (sub, lanes), 1)
    head = lax.broadcasted_iota(jnp.int32, (sub, lanes), 0)
    own = (lax.div(lane, CHUNK) == lax.div(head, ratio)) & (head < heads)
    pos_in = jnp.where(own, lax.rem(lane, CHUNK), 1 << 20)

    line = lax.broadcasted_iota(jnp.int32, (CHUNK, sub, lanes), 0)
    mine = line == pos_in[None]
    blocks = [slice(b0, b0 + CHUNK) for b0 in range(0, batch, CHUNK)]
    for rows in blocks:
        q = q_buf[rows].reshape(CHUNK * sub, head_dim).astype(BF16)
        s = lax.dot_general(q, kn_buf[:, rows].reshape(lanes, head_dim), (((1,), (1,)), ((), ())), preferred_element_type=F32) * scale
        s = jnp.where(mine, s.reshape(CHUNK, sub, lanes), MASK_VALUE)
        fresh[rows] = s
        peak[rows] = s

    def wait_step(ring, sem, step):
        at = lax.rem(step, ring_steps)
        pltpu.make_async_copy(ring.at[pl.ds(0, UNROLL)], ring.at[pl.ds(at * UNROLL, UNROLL)], sem.at[at]).wait()

    def refill(cache, ring, sem, step):
        @pl.when(step + ring_steps < steps)
        def _():
            @pl.loop(0, UNROLL)
            def _(u):
                item_copy(cache, ring, sem, (step + ring_steps) * UNROLL + u).start()

    def item(step, u, listed):
        k = step * UNROLL + u
        if listed:
            return k, item_seq[k], lax.rem(item_seq[k], batch), item_pos[k]
        return k, k, k, 0

    def score_step(step, listed):
        base = lax.rem(step, ring_steps) * UNROLL
        found = []
        for u in range(UNROLL):
            k, seq, row, pos = item(step, u, listed)
            keys = k_ring[base + u].reshape(lanes, head_dim)
            s = lax.dot_general(q_buf[row].astype(BF16), keys, (((1,), (1,)), ((), ())), preferred_element_type=F32) * scale
            s = jnp.where(pos_in < lengths[row] - pos, s, MASK_VALUE)
            score[k] = s
            found.append((seq, s))
        for seq, s in found:
            peak[seq] = jnp.maximum(peak[seq], s)

    def value_step(step, listed):
        base = lax.rem(step, ring_steps) * UNROLL
        found = []
        for u in range(UNROLL):
            k, seq, row, pos = item(step, u, listed)
            p = jnp.exp(score[k] - peak[seq])
            values = v_ring[base + u].reshape(lanes, head_dim)
            found.append((seq, p, jnp.dot(p.astype(BF16), values, preferred_element_type=F32)))
        for seq, p, o in found:
            total[seq] = total[seq] + p
            mixed[seq] = mixed[seq] + o

    def u_copy(p):
        cols = pl.ds(pl.multiple_of(p * half, half), half)
        return pltpu.make_async_copy(u_out.at[:, cols], packed.at[:, cols], out_sem.at[1])

    def wait_piece(p):
        slot = lax.rem(lead + p, SLOTS)
        pltpu.make_async_copy(w_gate.at[:, pl.ds(0, TILE)], w_buf.at[slot], w_sem.at[slot]).wait()

    def piece(p):
        prod = jnp.dot(h_buf[...], w_buf[lax.rem(lead + p, SLOTS)], preferred_element_type=F32)
        u_out[:, pl.ds(pl.multiple_of(p * half, half), half)] = (jax.nn.silu(prod[:, :half]) * prod[:, half:]).astype(BF16)

    def after_piece(p):
        u_copy(p).start()

        @pl.when(p + SLOTS < pieces)
        def _():
            start_piece(p + SLOTS, lax.rem(lead + p, SLOTS))

    def both(attend_step, cache, ring, sem, p0, p1):
        @pl.loop(0, first_steps)
        def _(s):
            wait_step(ring, sem, s)
            wait_piece(p0 + s)
            attend_step(s, False)
            piece(p0 + s)
            refill(cache, ring, sem, s)
            after_piece(p0 + s)

        fused = jnp.minimum(steps, p1 - p0)

        @pl.loop(first_steps, fused)
        def _(s):
            wait_step(ring, sem, s)
            wait_piece(p0 + s)
            attend_step(s, True)
            piece(p0 + s)
            refill(cache, ring, sem, s)
            after_piece(p0 + s)

        @pl.loop(fused, steps)
        def _(s):
            wait_step(ring, sem, s)
            attend_step(s, True)
            refill(cache, ring, sem, s)

        return p0 + fused

    reached = both(score_step, k_cache, k_ring, k_sem, 0, PIECES_SCORE)

    @pl.loop(reached, PIECES_SCORE)
    def _(p):
        wait_piece(p)
        piece(p)
        after_piece(p)

    for rows in blocks:
        top = jnp.broadcast_to(jnp.max(peak[rows], axis=-1, keepdims=True), (CHUNK, sub, lanes))
        peak[rows] = top
        p = jnp.exp(fresh[rows] - top)
        total[rows] = p
        o = jnp.dot(p.reshape(CHUNK * sub, lanes).astype(BF16), vn_buf[:, rows].reshape(lanes, head_dim), preferred_element_type=F32)
        mixed[rows] = o.reshape(CHUNK, sub, head_dim)

    reached = both(value_step, v_cache, v_ring, v_sem, PIECES_SCORE, PIECES_SCORE + PIECES_VALUE)

    q_buf[...] = mixed[:batch] / jnp.sum(total[:batch], axis=-1, keepdims=True)
    for h in range(heads):
        o_out[:, h * head_dim:(h + 1) * head_dim] = q_buf[:, h, :].astype(BF16)
    o_copy = pltpu.make_async_copy(o_out, packed.at[:, o_at:kv_at], out_sem.at[2])
    o_copy.start()

    @pl.loop(reached, pieces)
    def _(p):
        wait_piece(p)
        piece(p)
        after_piece(p)

    kv_copy.wait()
    o_copy.wait()
    for copy in x_copies:
        copy.wait()
    pltpu.make_async_copy(u_out, packed.at[:, :width], out_sem.at[1]).wait()


def front(tokens, lengths, k_cache, v_cache, norm_gain, w_query, w_key, w_value, w_gate, w_up, groups):
    batch, model_dim = tokens.shape
    kv_heads, context, head_dim = k_cache.shape[1:]
    local_kv = kv_heads // groups
    q_dim = w_query.shape[1]
    width = w_gate.shape[1]
    half_freq = np.exp(np.arange(head_dim // 2) * (-2.0 * math.log(ROPE_BASE) / head_dim))
    freq = jnp.asarray(np.concatenate([half_freq, half_freq])[None, :], F32)
    items = batch * (context // CHUNK) + UNROLL
    lanes = local_kv * CHUNK
    dma = pltpu.SemaphoreType.DMA
    hbm = pl.BlockSpec(memory_space=pltpu.HBM)
    smem = pl.BlockSpec(memory_space=pltpu.SMEM)
    return pl.pallas_call(
        front_kernel,
        out_shape=jax.ShapeDtypeStruct((batch, width + q_dim + 2 * local_kv * head_dim + model_dim // 4), BF16),
        in_specs=[smem] + [hbm] * 10,
        out_specs=hbm,
        scratch_shapes=[
            pltpu.VMEM((batch, model_dim), BF16),
            pltpu.VMEM((batch, model_dim), BF16),
            pltpu.VMEM((SLOTS, model_dim, TILE), BF16),
            pltpu.VMEM((RING, local_kv, CHUNK, head_dim), BF16),
            pltpu.VMEM((RING, local_kv, CHUNK, head_dim), BF16),
            pltpu.VMEM((batch, 8, head_dim), F32),
            pltpu.VMEM((local_kv, batch, head_dim), BF16),
            pltpu.VMEM((local_kv, batch, head_dim), BF16),
            pltpu.VMEM((batch, 8, lanes), F32),
            pltpu.VMEM((items, 8, lanes), F32),
            pltpu.VMEM((batch + 1, 8, lanes), F32),
            pltpu.VMEM((batch + 1, 8, lanes), F32),
            pltpu.VMEM((batch + 1, 8, head_dim), F32),
            pltpu.VMEM((batch, head_dim), F32),
            pltpu.VMEM((2, batch, head_dim), F32),
            pltpu.VMEM((model_dim,), BF16),
            pltpu.VMEM((1, head_dim), F32),
            pltpu.VMEM((batch, q_dim), BF16),
            pltpu.VMEM((batch, 2 * local_kv * head_dim), BF16),
            pltpu.VMEM((batch, width), BF16),
            pltpu.SMEM((items,), jnp.int32),
            pltpu.SMEM((items,), jnp.int32),
            dma((7,)), dma((3,)), dma((SLOTS,)), dma((RING // UNROLL,)), dma((RING // UNROLL,)),
        ],
        compiler_params=pltpu.CompilerParams(vmem_limit_bytes=VMEM_BYTES),
        name="front",
    )(lengths, tokens, norm_gain, freq, k_cache, v_cache, w_query, w_key, w_value, w_gate, w_up)


def back_kernel(packed, w_down, w_out,
                y_out, key_out, value_out, _,
                u_buf, o_buf, kv_buf, x_buf, w_buf, wo_buf, part, from_sib, to_cross, from_cross, y_buf, kv_in, head_buf,
                in_sem, w_sem, wo_sem, kv_send, kv_recv, s1_send, s1_recv, s2_send, s2_recv,
                yc_send, yc_recv, ys_send, ys_recv, yr_send, yr_recv):
    me = lax.axis_index('model')
    core = lax.rem(me, 2)
    chip = lax.div(me, 2)
    sib = chip * 2 + (1 - core)
    cross = (1 - chip) * 2 + core
    diag = (1 - chip) * 2 + (1 - core)
    n_out = w_down.shape[1] // TILE
    head_dim = head_buf.shape[2]
    local_kv = kv_buf.shape[2] // (2 * head_dim)
    lag_sib, lag_cross, lag_relay, lag_store = LAGS

    barrier = pltpu.get_barrier_semaphore()
    for peer in (sib, cross, diag):
        pl.semaphore_signal(barrier, inc=1, device_id={'model': peer}, device_id_type=MESH)

    def cols(tile):
        return pl.ds(pl.multiple_of(tile * TILE, TILE), TILE)

    def down_copy(c):
        return pltpu.make_async_copy(w_down.at[:, cols(c)], w_buf.at[c], w_sem.at[c])

    def remote(src, dst, send, recv, peer):
        return pltpu.make_async_remote_copy(src_ref=src, dst_ref=dst, send_sem=send, recv_sem=recv,
                                            device_id={'model': peer}, device_id_type=MESH)

    def out_copy(c):
        return pltpu.make_async_copy(w_out.at[:, cols(c)], wo_buf.at[c], wo_sem.at[c])

    devices, rows = kv_buf.shape[:2]
    width, q_dim = u_buf.shape[1], o_buf.shape[1]
    kv_at = width + q_dim
    x_at = kv_at + kv_buf.shape[2]
    x_part = x_buf.shape[2]
    o_copy = pltpu.make_async_copy(packed.at[:, width:kv_at], o_buf, in_sem.at[0])
    u_copy = pltpu.make_async_copy(packed.at[:, :width], u_buf, in_sem.at[1])
    kv_copies = [pltpu.make_async_copy(packed.at[n * rows:(n + 1) * rows, kv_at:x_at], kv_buf.at[n], in_sem.at[2 + n]) for n in range(devices)]
    x_copies = [pltpu.make_async_copy(packed.at[n * rows:(n + 1) * rows, x_at:x_at + x_part], x_buf.at[n], in_sem.at[2 + devices + n])
                for n in range(devices)]
    for copy in (o_copy, u_copy, out_copy(0), down_copy(0), *kv_copies, *x_copies):
        copy.start()

    @pl.loop(1, n_out)
    def _(c):
        out_copy(c).start()
        down_copy(c).start()

    for copy in (o_copy, u_copy):
        copy.wait()

    kv_peers = (sib, cross, diag)

    def kv_copy(n):
        return remote(kv_buf.at[kv_peers[n]], kv_in.at[me], kv_send.at[n], kv_recv.at[n], kv_peers[n])

    def sib_send(c):
        return remote(part.at[c, :, 1 - core], from_sib.at[c], s1_send, s1_recv.at[c], sib)

    def cross_send(c):
        return remote(to_cross.at[c], from_cross.at[c], s2_send, s2_recv.at[c], cross)

    def y_cross(c):
        return remote(y_buf.at[c, me], y_buf.at[c, me], yc_send, yc_recv.at[c], cross)

    def y_sib(c):
        return remote(y_buf.at[c, me], y_buf.at[c, me], ys_send, ys_recv.at[c], sib)

    def y_relay(c):
        return remote(y_buf.at[c, cross], y_buf.at[c, cross], yr_send, yr_recv.at[c], sib)

    def product(c):
        out_copy(c).wait()
        total = jnp.dot(o_buf[...], wo_buf[c], preferred_element_type=F32)
        down_copy(c).wait()
        total += jnp.dot(u_buf[...], w_buf[c], preferred_element_type=F32)
        part[c] = total.reshape(part.shape[1:])

    product(0)
    for copy in (*kv_copies, *x_copies):
        copy.wait()
    pl.semaphore_wait(barrier, 3)
    sib_send(0).start()
    for n in range(3):
        kv_copy(n).start()

    @pl.loop(1, n_out + lag_store)
    def _(i):
        @pl.when(i < n_out)
        def _():
            product(i)
            sib_send(i).start()

        @pl.when((i >= lag_sib) & (i < n_out + lag_sib))
        def _():
            c = i - lag_sib
            sib_send(c).wait_recv()
            to_cross[c] = part[c, 1 - chip, core] + from_sib[c, 1 - chip]
            cross_send(c).start()

        @pl.when((i >= lag_cross) & (i < n_out + lag_cross))
        def _():
            c = i - lag_cross
            cross_send(c).wait_recv()
            total = part[c, chip, core] + from_sib[c, chip] + from_cross[c]
            x = x_buf[lax.div(c * TILE, x_part), :, pl.ds(pl.multiple_of(lax.rem(c * TILE, x_part), TILE), TILE)]
            y_buf[c, me] = (x.astype(F32) + total).astype(BF16)
            y_cross(c).start()
            y_sib(c).start()

        @pl.when((i >= lag_relay) & (i < n_out + lag_relay))
        def _():
            c = i - lag_relay
            y_cross(c).wait_recv()
            y_relay(c).start()

        @pl.when(i == n_out)
        def _():
            for n in range(3):
                kv_copy(n).wait_recv()
            kv_in[me] = kv_buf[me]
            for half, out in enumerate((key_out, value_out)):
                for source in range(kv_in.shape[0]):
                    for g in range(local_kv):
                        start = (half * local_kv + g) * head_dim
                        head_buf[:, source * local_kv + g, :] = kv_in[source, :, start:start + head_dim].astype(F32)
                out[...] = head_buf[...].astype(BF16)

        @pl.when(i >= lag_store)
        def _():
            c = i - lag_store
            y_sib(c).wait_recv()
            y_relay(c).wait_recv()
            y_out[:, :, cols(c)] = y_buf[c]

    for n in range(3):
        kv_copy(n).wait_send()
    remote(part.at[:, :, 0], from_sib, s1_send, s1_recv.at[0], sib).wait_send()
    remote(to_cross, from_cross, s2_send, s2_recv.at[0], cross).wait_send()
    for sem in (yc_send, ys_send, yr_send):
        remote(y_buf.at[:, 0], y_buf.at[:, 0], sem, yc_recv.at[0], sib).wait_send()


def back(packed, w_down, w_out, kv_heads, head_dim, devices):
    batch = packed.shape[0]
    width, model_dim = w_down.shape
    q_dim = w_out.shape[0]
    rows = batch // devices
    n_out = model_dim // TILE
    kv_width = 2 * (kv_heads // devices) * head_dim
    dma = pltpu.SemaphoreType.DMA
    hbm = pl.BlockSpec(memory_space=pltpu.HBM)
    vmem = pl.BlockSpec(memory_space=pltpu.VMEM)
    y, key_out, value_out, _ = pl.pallas_call(
        back_kernel,
        out_shape=(jax.ShapeDtypeStruct((devices, rows, model_dim), BF16),
                   jax.ShapeDtypeStruct((rows, kv_heads, head_dim), BF16),
                   jax.ShapeDtypeStruct((rows, kv_heads, head_dim), BF16),
                   jax.ShapeDtypeStruct(packed.shape, BF16)),
        in_specs=[hbm] * 3,
        out_specs=(vmem, vmem, vmem, hbm),
        input_output_aliases={0: 3},
        scratch_shapes=[
            pltpu.VMEM((batch, width), BF16),
            pltpu.VMEM((batch, q_dim), BF16),
            pltpu.VMEM((devices, rows, kv_width), BF16),
            pltpu.VMEM((4, rows, model_dim // 4), BF16),
            pltpu.VMEM((n_out, width, TILE), BF16),
            pltpu.VMEM((n_out, q_dim, TILE), BF16),
            pltpu.VMEM((n_out, 2, 2, rows, TILE), F32),
            pltpu.VMEM((n_out, 2, rows, TILE), F32),
            pltpu.VMEM((n_out, rows, TILE), F32),
            pltpu.VMEM((n_out, rows, TILE), F32),
            pltpu.VMEM((n_out, devices, rows, TILE), BF16),
            pltpu.VMEM((devices, rows, kv_width), BF16),
            pltpu.VMEM((rows, kv_heads, head_dim), F32),
            dma((2 + 2 * devices,)), dma((n_out,)), dma((n_out,)), dma((3,)), dma((3,)),
        ] + [dma, dma((n_out,))] * 5,
        compiler_params=pltpu.CompilerParams(collective_id=0, has_side_effects=True, vmem_limit_bytes=VMEM_BYTES - RESULT_BYTES),
        name="back",
    )(packed, w_down, w_out)
    return finish(y.reshape(batch, model_dim), key_out, value_out)


def finish_kernel(*refs):
    half = (len(refs) - 1) // 2
    copies = [pltpu.make_async_copy(refs[n], refs[half + n], refs[-1].at[n]) for n in range(half)]
    for copy in copies:
        copy.start()
    for copy in copies:
        copy.wait()


def finish(*arrays):
    return pl.pallas_call(
        finish_kernel,
        out_shape=tuple(jax.ShapeDtypeStruct(a.shape, a.dtype) for a in arrays),
        in_specs=[pl.BlockSpec(memory_space=pltpu.VMEM)] * len(arrays),
        out_specs=tuple(pl.BlockSpec(memory_space=pltpu.HBM) for _ in arrays),
        scratch_shapes=[pltpu.SemaphoreType.DMA((len(arrays),))],
        compiler_params=pltpu.CompilerParams(vmem_limit_bytes=4 * 2 ** 20),
        name="finish",
    )(*arrays)


def solution(mesh):
    groups = mesh.shape['model']

    def local_step(tokens, lengths, k_cache, v_cache, norm_gain, w_query, w_key, w_value, w_out, w_gate, w_up, w_down):
        kv_heads, _, head_dim = k_cache.shape[1:]
        packed = front(tokens, lengths, k_cache, v_cache, norm_gain, w_query, w_key, w_value, w_gate, w_up, groups)
        return back(packed, w_down, w_out, kv_heads, head_dim, groups)

    in_specs = (P('replica', None), P('replica'), P('replica', None, None, None), P('replica', None, None, None), P(None), P(None, 'model'), P(None, None), P(None, None), P('model', None), P(None, 'model'), P(None, 'model'), P('model', None))
    out_specs = (P('replica', None), P(('replica', 'model'), None, None), P(('replica', 'model'), None, None))
    return jax.shard_map(local_step, mesh=mesh, in_specs=in_specs, out_specs=out_specs, check_vma=False)
```

```python
import functools
import math

import jax
import jax.numpy as jnp
import numpy as np
from jax import lax
from jax.experimental import pallas as pl
from jax.experimental.pallas import tpu as pltpu
from jax.sharding import PartitionSpec as P

ROPE_BASE = 10000.0
NORM_EPS = 1e-6
MASK_VALUE = -1e30
MESH = pl.DeviceIdType.MESH
F32 = jnp.float32
BF16 = jnp.bfloat16
TILE = 256
SLOTS = 8
LEAD_NOW = 2
PIECES_NOW = 1
LAGS = (1, 6, 11, 13)
CHUNK = 64
UNROLL = 16
VMEM_BYTES = 67_043_328
RESULT_BYTES = 12_000_000
PIECES_SCORE = 13
PIECES_VALUE = 11
RING = 128


def front_kernel(lengths, tokens, gain_hbm, freq_hbm, k_cache, v_cache, w_query, w_key, w_value, w_gate, w_up,
                 packed,
                 x_buf, h_buf, w_buf, k_first, v_first, k_more, v_more, q_buf, kn_buf, vn_buf, fresh, score, peak, total, mixed, angle, rot,
                 gain, freq, o_out, kv_out, u_out,
                 item_seq, item_pos, out_sem, x_sem, w_sem, kf_sem, vf_sem, km_sem, vm_sem):
    batch, model_dim = tokens.shape
    head_dim = freq.shape[1]
    local_kv = kv_out.shape[1] // (2 * head_dim)
    heads = o_out.shape[1] // head_dim
    ratio = heads // local_kv
    q_tiles = w_query.shape[1] // TILE
    lead = q_tiles + 2
    half = TILE // 2
    pieces = w_gate.shape[1] // half
    ring_steps = RING // UNROLL
    first_steps = batch // UNROLL
    scale = head_dim ** -0.5
    me = lax.axis_index('model')
    local = pl.ds(me * local_kv, local_kv)
    lanes = local_kv * CHUNK

    def w_copy(src, tile, t):
        return pltpu.make_async_copy(src.at[:, pl.ds(pl.multiple_of(tile * TILE, TILE), TILE)], w_buf.at[t], w_sem.at[t])

    def start_piece(p, slot):
        for n, src in enumerate((w_gate, w_up)):
            pltpu.make_async_copy(src.at[:, pl.ds(pl.multiple_of(p * half, half), half)],
                                  w_buf.at[slot, :, n * half:(n + 1) * half], w_sem.at[slot]).start()

    def first_copy(cache, first, sem, step):
        rows = pl.ds(step * UNROLL, UNROLL)
        return pltpu.make_async_copy(cache.at[rows, local, pl.ds(0, CHUNK)], first.at[rows], sem.at[step])

    def start_items(cache, more, sem, step):
        at = lax.rem(step, ring_steps)
        for u in range(UNROLL):
            k = step * UNROLL + u
            pltpu.make_async_copy(cache.at[lax.rem(item_seq[k], batch), local, pl.ds(pl.multiple_of(item_pos[k], CHUNK), CHUNK)],
                                  more.at[at * UNROLL + u], sem.at[at]).start()

    x_copy = pltpu.make_async_copy(tokens, x_buf, x_sem.at[0])
    gain_copy = pltpu.make_async_copy(gain_hbm, gain, x_sem.at[1])
    freq_copy = pltpu.make_async_copy(freq_hbm, freq, x_sem.at[2])
    for copy in (freq_copy, x_copy, gain_copy):
        copy.start()
    lead_copies = [w_copy(w_key, me, 0), w_copy(w_value, me, 1)] + [w_copy(w_query, t, 2 + t) for t in range(q_tiles)]
    for copy in lead_copies[:LEAD_NOW]:
        copy.start()

    def second(i, k):
        for r in range(UNROLL):
            seq = i * UNROLL + r
            item_seq[k] = seq
            item_pos[k] = CHUNK
            k = k + (lengths[seq] > CHUNK).astype(jnp.int32)
        return k

    begin, end = 0, lax.fori_loop(0, batch // UNROLL, second, 0)
    for c in range(2, k_cache.shape[2] // CHUNK):
        def further(i, k):
            for r in range(4):
                at = begin + i * 4 + r
                seq = lax.rem(jnp.maximum(item_seq[at], 0), batch)
                item_seq[k] = seq
                item_pos[k] = c * CHUNK
                k = k + ((lengths[seq] > c * CHUNK) & (at < end)).astype(jnp.int32)
            return k

        begin, end = end, lax.fori_loop(0, lax.div(end - begin + 3, 4), further, end)
    steps = lax.div(end + (UNROLL - 1), UNROLL)

    for u in range(UNROLL):
        item_seq[end + u] = batch
        item_pos[end + u] = 0

    for copy in lead_copies[LEAD_NOW:]:
        copy.start()
    for step in range(first_steps):
        first_copy(k_cache, k_first, kf_sem, step).start()
    freq_copy.wait()

    @pl.loop(0, batch // 8)
    def _(i):
        for r in range(8):
            angle[pl.ds(i * 8 + r, 1), :] = lengths[i * 8 + r].astype(F32) * freq[...]

    first = lax.broadcasted_iota(jnp.int32, (batch, head_dim), 1) < head_dim // 2
    rot[0] = jnp.cos(angle[...])
    rot[1] = jnp.where(first, -jnp.sin(angle[...]), jnp.sin(angle[...]))
    q_buf[...] = jnp.zeros(q_buf.shape, F32)

    x_copy.wait()
    gain_copy.wait()
    for p in range(PIECES_NOW):
        start_piece(p, lead + p)
    x = x_buf[...].astype(F32)
    mean_sq = jnp.mean(x * x, axis=-1, keepdims=True)
    h_buf[...] = (x * lax.rsqrt(mean_sq + NORM_EPS) * gain[...].reshape(1, model_dim).astype(F32)).astype(BF16)

    def rope(a):
        return a * rot[0] + pltpu.roll(a, head_dim // 2, 1) * rot[1]

    for t, copy in enumerate(lead_copies):
        copy.wait()
        prod = jnp.dot(h_buf[...], w_buf[t], preferred_element_type=F32)
        if t == 0:
            for p in range(PIECES_NOW, SLOTS - lead):
                start_piece(p, lead + p)
        if t == 4:
            for step in range(first_steps):
                first_copy(v_cache, v_first, vf_sem, step).start()
        start_piece(SLOTS - lead + t, t)
        for j in range(TILE // head_dim):
            a = prod[:, j * head_dim:(j + 1) * head_dim]
            if t >= 2:
                q_buf[:, (t - 2) * (TILE // head_dim) + j, :] = rope(a).astype(BF16).astype(F32)
            else:
                a = (rope(a) if t == 0 else a).astype(BF16)
                col = (t * local_kv + j) * head_dim
                kv_out[:, col:col + head_dim] = a
                (kn_buf, vn_buf)[t][j] = a
    width = u_out.shape[1]
    o_at, kv_at = width, width + heads * head_dim
    x_at = kv_at + kv_out.shape[1]
    kv_copy = pltpu.make_async_copy(kv_out, packed.at[:, kv_at:x_at], out_sem.at[0])
    kv_copy.start()
    quarter = batch // 4
    x_part = model_dim // 4
    x_rows = pl.ds(pl.multiple_of(me * quarter, quarter), quarter)
    x_copies = [pltpu.make_async_copy(x_buf.at[x_rows, n * x_part:(n + 1) * x_part],
                                      packed.at[n * quarter:(n + 1) * quarter, x_at:x_at + x_part], out_sem.at[3 + n]) for n in range(4)]
    for copy in x_copies:
        copy.start()
    peak[batch] = jnp.full(peak.shape[1:], MASK_VALUE, F32)
    total[batch] = jnp.zeros(total.shape[1:], F32)
    mixed[batch] = jnp.zeros(mixed.shape[1:], F32)

    sub = q_buf.shape[1]
    lane = lax.broadcasted_iota(jnp.int32, (sub, lanes), 1)
    head = lax.broadcasted_iota(jnp.int32, (sub, lanes), 0)
    own = (lax.div(lane, CHUNK) == lax.div(head, ratio)) & (head < heads)
    pos_in = jnp.where(own, lax.rem(lane, CHUNK), 1 << 20)

    line = lax.broadcasted_iota(jnp.int32, (CHUNK, sub, lanes), 0)
    mine = line == pos_in[None]
    blocks = [slice(b0, b0 + CHUNK) for b0 in range(0, batch, CHUNK)]
    for rows in blocks:
        q = q_buf[rows].reshape(CHUNK * sub, head_dim).astype(BF16)
        s = lax.dot_general(q, kn_buf[:, rows].reshape(lanes, head_dim), (((1,), (1,)), ((), ())), preferred_element_type=F32) * scale
        s = jnp.where(mine, s.reshape(CHUNK, sub, lanes), MASK_VALUE)
        fresh[rows] = s
        peak[rows] = s

    def wait_first(first, sem, step):
        pltpu.make_async_copy(first.at[pl.ds(0, UNROLL)], first.at[pl.ds(step * UNROLL, UNROLL)], sem.at[step]).wait()

    def wait_more(more, sem, step):
        at = lax.rem(step, ring_steps)
        pltpu.make_async_copy(more.at[pl.ds(0, UNROLL)], more.at[pl.ds(at * UNROLL, UNROLL)], sem.at[at]).wait()

    def refill(cache, more, sem, step):
        @pl.when(step + ring_steps < steps)
        def _():
            start_items(cache, more, sem, step + ring_steps)

    def item(step, u, listed):
        k = step * UNROLL + u
        if listed:
            return batch + k, lax.rem(step, ring_steps) * UNROLL + u, item_seq[k], lax.rem(item_seq[k], batch), item_pos[k]
        return k, k, k, k, 0

    def score_step(step, listed):
        ring = k_more if listed else k_first
        found = []
        for u in range(UNROLL):
            k, at, seq, row, pos = item(step, u, listed)
            keys = ring[at].reshape(lanes, head_dim)
            s = lax.dot_general(q_buf[row].astype(BF16), keys, (((1,), (1,)), ((), ())), preferred_element_type=F32) * scale
            s = jnp.where(pos_in < lengths[row] - pos, s, MASK_VALUE)
            score[k] = s
            found.append((seq, s))
        for seq, s in found:
            peak[seq] = jnp.maximum(peak[seq], s)

    def value_step(step, listed):
        ring = v_more if listed else v_first
        found = []
        for u in range(UNROLL):
            k, at, seq, row, pos = item(step, u, listed)
            p = jnp.exp(score[k] - peak[seq])
            values = ring[at].reshape(lanes, head_dim)
            found.append((seq, p, jnp.dot(p.astype(BF16), values, preferred_element_type=F32)))
        for seq, p, o in found:
            total[seq] = total[seq] + p
            mixed[seq] = mixed[seq] + o

    def u_copy(p):
        cols = pl.ds(pl.multiple_of(p * half, half), half)
        return pltpu.make_async_copy(u_out.at[:, cols], packed.at[:, cols], out_sem.at[1])

    def wait_piece(p):
        slot = lax.rem(lead + p, SLOTS)
        pltpu.make_async_copy(w_gate.at[:, pl.ds(0, TILE)], w_buf.at[slot], w_sem.at[slot]).wait()

    def piece(p):
        prod = jnp.dot(h_buf[...], w_buf[lax.rem(lead + p, SLOTS)], preferred_element_type=F32)
        u_out[:, pl.ds(pl.multiple_of(p * half, half), half)] = (jax.nn.silu(prod[:, :half]) * prod[:, half:]).astype(BF16)

    def after_piece(p):
        u_copy(p).start()

        @pl.when(p + SLOTS < pieces)
        def _():
            start_piece(p + SLOTS, lax.rem(lead + p, SLOTS))

    def both(attend_step, cache, first, first_sem, more, more_sem, p0, p1):
        fetching = jnp.minimum(steps, first_steps)
        fused = jnp.minimum(steps, p1 - p0 - first_steps)

        def first_step(s, fetch):
            wait_first(first, first_sem, s)
            wait_piece(p0 + s)
            if fetch:
                start_items(cache, more, more_sem, s)
            attend_step(s, False)
            piece(p0 + s)
            after_piece(p0 + s)

        @pl.loop(0, fetching)
        def _(s):
            first_step(s, True)

        @pl.loop(fetching, first_steps)
        def _(s):
            first_step(s, False)

        @pl.loop(0, fused)
        def _(s):
            wait_more(more, more_sem, s)
            wait_piece(p0 + first_steps + s)
            attend_step(s, True)
            piece(p0 + first_steps + s)
            refill(cache, more, more_sem, s)
            after_piece(p0 + first_steps + s)

        @pl.loop(fused, steps)
        def _(s):
            wait_more(more, more_sem, s)
            attend_step(s, True)
            refill(cache, more, more_sem, s)

        return p0 + first_steps + fused

    reached = both(score_step, k_cache, k_first, kf_sem, k_more, km_sem, 0, PIECES_SCORE)

    @pl.loop(reached, PIECES_SCORE)
    def _(p):
        wait_piece(p)
        piece(p)
        after_piece(p)

    for rows in blocks:
        top = jnp.broadcast_to(jnp.max(peak[rows], axis=-1, keepdims=True), (CHUNK, sub, lanes))
        peak[rows] = top
        p = jnp.exp(fresh[rows] - top)
        total[rows] = p
        o = jnp.dot(p.reshape(CHUNK * sub, lanes).astype(BF16), vn_buf[:, rows].reshape(lanes, head_dim), preferred_element_type=F32)
        mixed[rows] = o.reshape(CHUNK, sub, head_dim)

    reached = both(value_step, v_cache, v_first, vf_sem, v_more, vm_sem, PIECES_SCORE, PIECES_SCORE + PIECES_VALUE)

    q_buf[...] = mixed[:batch] / jnp.sum(total[:batch], axis=-1, keepdims=True)
    for h in range(heads):
        o_out[:, h * head_dim:(h + 1) * head_dim] = q_buf[:, h, :].astype(BF16)
    o_copy = pltpu.make_async_copy(o_out, packed.at[:, o_at:kv_at], out_sem.at[2])
    o_copy.start()

    @pl.loop(reached, pieces)
    def _(p):
        wait_piece(p)
        piece(p)
        after_piece(p)

    kv_copy.wait()
    o_copy.wait()
    for copy in x_copies:
        copy.wait()
    pltpu.make_async_copy(u_out, packed.at[:, :width], out_sem.at[1]).wait()


def front(tokens, lengths, k_cache, v_cache, norm_gain, w_query, w_key, w_value, w_gate, w_up, groups):
    batch, model_dim = tokens.shape
    kv_heads, context, head_dim = k_cache.shape[1:]
    local_kv = kv_heads // groups
    q_dim = w_query.shape[1]
    width = w_gate.shape[1]
    half_freq = np.exp(np.arange(head_dim // 2) * (-2.0 * math.log(ROPE_BASE) / head_dim))
    freq = jnp.asarray(np.concatenate([half_freq, half_freq])[None, :], F32)
    items = batch * (context // CHUNK) + 2 * UNROLL
    lanes = local_kv * CHUNK
    dma = pltpu.SemaphoreType.DMA
    hbm = pl.BlockSpec(memory_space=pltpu.HBM)
    smem = pl.BlockSpec(memory_space=pltpu.SMEM)
    return pl.pallas_call(
        front_kernel,
        out_shape=jax.ShapeDtypeStruct((batch, width + q_dim + 2 * local_kv * head_dim + model_dim // 4), BF16),
        in_specs=[smem] + [hbm] * 10,
        out_specs=hbm,
        scratch_shapes=[
            pltpu.VMEM((batch, model_dim), BF16),
            pltpu.VMEM((batch, model_dim), BF16),
            pltpu.VMEM((SLOTS, model_dim, TILE), BF16),
            pltpu.VMEM((batch, local_kv, CHUNK, head_dim), BF16),
            pltpu.VMEM((batch, local_kv, CHUNK, head_dim), BF16),
            pltpu.VMEM((RING, local_kv, CHUNK, head_dim), BF16),
            pltpu.VMEM((RING, local_kv, CHUNK, head_dim), BF16),
            pltpu.VMEM((batch, 8, head_dim), F32),
            pltpu.VMEM((local_kv, batch, head_dim), BF16),
            pltpu.VMEM((local_kv, batch, head_dim), BF16),
            pltpu.VMEM((batch, 8, lanes), F32),
            pltpu.VMEM((items, 8, lanes), F32),
            pltpu.VMEM((batch + 1, 8, lanes), F32),
            pltpu.VMEM((batch + 1, 8, lanes), F32),
            pltpu.VMEM((batch + 1, 8, head_dim), F32),
            pltpu.VMEM((batch, head_dim), F32),
            pltpu.VMEM((2, batch, head_dim), F32),
            pltpu.VMEM((model_dim,), BF16),
            pltpu.VMEM((1, head_dim), F32),
            pltpu.VMEM((batch, q_dim), BF16),
            pltpu.VMEM((batch, 2 * local_kv * head_dim), BF16),
            pltpu.VMEM((batch, width), BF16),
            pltpu.SMEM((items,), jnp.int32),
            pltpu.SMEM((items,), jnp.int32),
            dma((7,)), dma((3,)), dma((SLOTS,)), dma((batch // UNROLL,)), dma((batch // UNROLL,)),
            dma((RING // UNROLL,)), dma((RING // UNROLL,)),
        ],
        compiler_params=pltpu.CompilerParams(vmem_limit_bytes=VMEM_BYTES),
        name="front",
    )(lengths, tokens, norm_gain, freq, k_cache, v_cache, w_query, w_key, w_value, w_gate, w_up)


def back_kernel(packed, w_down, w_out,
                y_out, key_out, value_out, _,
                u_buf, o_buf, kv_buf, x_buf, w_buf, wo_buf, part, from_sib, to_cross, from_cross, y_buf, kv_in, head_buf,
                in_sem, w_sem, wo_sem, kv_send, kv_recv, s1_send, s1_recv, s2_send, s2_recv,
                yc_send, yc_recv, ys_send, ys_recv, yr_send, yr_recv):
    me = lax.axis_index('model')
    core = lax.rem(me, 2)
    chip = lax.div(me, 2)
    sib = chip * 2 + (1 - core)
    cross = (1 - chip) * 2 + core
    diag = (1 - chip) * 2 + (1 - core)
    n_out = w_down.shape[1] // TILE
    head_dim = head_buf.shape[2]
    local_kv = kv_buf.shape[2] // (2 * head_dim)
    lag_sib, lag_cross, lag_relay, lag_store = LAGS

    barrier = pltpu.get_barrier_semaphore()
    for peer in (sib, cross, diag):
        pl.semaphore_signal(barrier, inc=1, device_id={'model': peer}, device_id_type=MESH)

    def cols(tile):
        return pl.ds(pl.multiple_of(tile * TILE, TILE), TILE)

    def down_copy(c):
        return pltpu.make_async_copy(w_down.at[:, cols(c)], w_buf.at[c], w_sem.at[c])

    def remote(src, dst, send, recv, peer):
        return pltpu.make_async_remote_copy(src_ref=src, dst_ref=dst, send_sem=send, recv_sem=recv,
                                            device_id={'model': peer}, device_id_type=MESH)

    def out_copy(c):
        return pltpu.make_async_copy(w_out.at[:, cols(c)], wo_buf.at[c], wo_sem.at[c])

    devices, rows = kv_buf.shape[:2]
    width, q_dim = u_buf.shape[1], o_buf.shape[1]
    kv_at = width + q_dim
    x_at = kv_at + kv_buf.shape[2]
    x_part = x_buf.shape[2]
    o_copy = pltpu.make_async_copy(packed.at[:, width:kv_at], o_buf, in_sem.at[0])
    u_copy = pltpu.make_async_copy(packed.at[:, :width], u_buf, in_sem.at[1])
    kv_copies = [pltpu.make_async_copy(packed.at[n * rows:(n + 1) * rows, kv_at:x_at], kv_buf.at[n], in_sem.at[2 + n]) for n in range(devices)]
    x_copies = [pltpu.make_async_copy(packed.at[n * rows:(n + 1) * rows, x_at:x_at + x_part], x_buf.at[n], in_sem.at[2 + devices + n])
                for n in range(devices)]
    for copy in (o_copy, u_copy, out_copy(0), down_copy(0), *kv_copies, *x_copies):
        copy.start()

    @pl.loop(1, n_out)
    def _(c):
        out_copy(c).start()
        down_copy(c).start()

    for copy in (o_copy, u_copy):
        copy.wait()

    kv_peers = (sib, cross, diag)

    def kv_copy(n):
        return remote(kv_buf.at[kv_peers[n]], kv_in.at[me], kv_send.at[n], kv_recv.at[n], kv_peers[n])

    def sib_send(c):
        return remote(part.at[c, :, 1 - core], from_sib.at[c], s1_send, s1_recv.at[c], sib)

    def cross_send(c):
        return remote(to_cross.at[c], from_cross.at[c], s2_send, s2_recv.at[c], cross)

    def y_cross(c):
        return remote(y_buf.at[c, me], y_buf.at[c, me], yc_send, yc_recv.at[c], cross)

    def y_sib(c):
        return remote(y_buf.at[c, me], y_buf.at[c, me], ys_send, ys_recv.at[c], sib)

    def y_relay(c):
        return remote(y_buf.at[c, cross], y_buf.at[c, cross], yr_send, yr_recv.at[c], sib)

    def product(c):
        out_copy(c).wait()
        total = jnp.dot(o_buf[...], wo_buf[c], preferred_element_type=F32)
        down_copy(c).wait()
        total += jnp.dot(u_buf[...], w_buf[c], preferred_element_type=F32)
        part[c] = total.reshape(part.shape[1:])

    product(0)
    for copy in (*kv_copies, *x_copies):
        copy.wait()
    pl.semaphore_wait(barrier, 3)
    sib_send(0).start()
    for n in range(3):
        kv_copy(n).start()

    @pl.loop(1, n_out + lag_store)
    def _(i):
        @pl.when(i < n_out)
        def _():
            product(i)
            sib_send(i).start()

        @pl.when((i >= lag_sib) & (i < n_out + lag_sib))
        def _():
            c = i - lag_sib
            sib_send(c).wait_recv()
            to_cross[c] = part[c, 1 - chip, core] + from_sib[c, 1 - chip]
            cross_send(c).start()

        @pl.when((i >= lag_cross) & (i < n_out + lag_cross))
        def _():
            c = i - lag_cross
            cross_send(c).wait_recv()
            total = part[c, chip, core] + from_sib[c, chip] + from_cross[c]
            x = x_buf[lax.div(c * TILE, x_part), :, pl.ds(pl.multiple_of(lax.rem(c * TILE, x_part), TILE), TILE)]
            y_buf[c, me] = (x.astype(F32) + total).astype(BF16)
            y_cross(c).start()
            y_sib(c).start()

        @pl.when((i >= lag_relay) & (i < n_out + lag_relay))
        def _():
            c = i - lag_relay
            y_cross(c).wait_recv()
            y_relay(c).start()

        @pl.when(i == n_out)
        def _():
            for n in range(3):
                kv_copy(n).wait_recv()
            kv_in[me] = kv_buf[me]
            for half, out in enumerate((key_out, value_out)):
                for source in range(kv_in.shape[0]):
                    for g in range(local_kv):
                        start = (half * local_kv + g) * head_dim
                        head_buf[:, source * local_kv + g, :] = kv_in[source, :, start:start + head_dim].astype(F32)
                out[...] = head_buf[...].astype(BF16)

        @pl.when(i >= lag_store)
        def _():
            c = i - lag_store
            y_sib(c).wait_recv()
            y_relay(c).wait_recv()
            y_out[:, :, cols(c)] = y_buf[c]

    for n in range(3):
        kv_copy(n).wait_send()
    remote(part.at[:, :, 0], from_sib, s1_send, s1_recv.at[0], sib).wait_send()
    remote(to_cross, from_cross, s2_send, s2_recv.at[0], cross).wait_send()
    for sem in (yc_send, ys_send, yr_send):
        remote(y_buf.at[:, 0], y_buf.at[:, 0], sem, yc_recv.at[0], sib).wait_send()


def back(packed, w_down, w_out, kv_heads, head_dim, devices):
    batch = packed.shape[0]
    width, model_dim = w_down.shape
    q_dim = w_out.shape[0]
    rows = batch // devices
    n_out = model_dim // TILE
    kv_width = 2 * (kv_heads // devices) * head_dim
    dma = pltpu.SemaphoreType.DMA
    hbm = pl.BlockSpec(memory_space=pltpu.HBM)
    vmem = pl.BlockSpec(memory_space=pltpu.VMEM)
    y, key_out, value_out, _ = pl.pallas_call(
        back_kernel,
        out_shape=(jax.ShapeDtypeStruct((devices, rows, model_dim), BF16),
                   jax.ShapeDtypeStruct((rows, kv_heads, head_dim), BF16),
                   jax.ShapeDtypeStruct((rows, kv_heads, head_dim), BF16),
                   jax.ShapeDtypeStruct(packed.shape, BF16)),
        in_specs=[hbm] * 3,
        out_specs=(vmem, vmem, vmem, hbm),
        input_output_aliases={0: 3},
        scratch_shapes=[
            pltpu.VMEM((batch, width), BF16),
            pltpu.VMEM((batch, q_dim), BF16),
            pltpu.VMEM((devices, rows, kv_width), BF16),
            pltpu.VMEM((4, rows, model_dim // 4), BF16),
            pltpu.VMEM((n_out, width, TILE), BF16),
            pltpu.VMEM((n_out, q_dim, TILE), BF16),
            pltpu.VMEM((n_out, 2, 2, rows, TILE), F32),
            pltpu.VMEM((n_out, 2, rows, TILE), F32),
            pltpu.VMEM((n_out, rows, TILE), F32),
            pltpu.VMEM((n_out, rows, TILE), F32),
            pltpu.VMEM((n_out, devices, rows, TILE), BF16),
            pltpu.VMEM((devices, rows, kv_width), BF16),
            pltpu.VMEM((rows, kv_heads, head_dim), F32),
            dma((2 + 2 * devices,)), dma((n_out,)), dma((n_out,)), dma((3,)), dma((3,)),
        ] + [dma, dma((n_out,))] * 5,
        compiler_params=pltpu.CompilerParams(collective_id=0, has_side_effects=True, vmem_limit_bytes=VMEM_BYTES - RESULT_BYTES),
        name="back",
    )(packed, w_down, w_out)
    return finish(y.reshape(batch, model_dim), key_out, value_out)


def finish_kernel(*refs):
    half = (len(refs) - 1) // 2
    copies = [pltpu.make_async_copy(refs[n], refs[half + n], refs[-1].at[n]) for n in range(half)]
    for copy in copies:
        copy.start()
    for copy in copies:
        copy.wait()


def finish(*arrays):
    return pl.pallas_call(
        finish_kernel,
        out_shape=tuple(jax.ShapeDtypeStruct(a.shape, a.dtype) for a in arrays),
        in_specs=[pl.BlockSpec(memory_space=pltpu.VMEM)] * len(arrays),
        out_specs=tuple(pl.BlockSpec(memory_space=pltpu.HBM) for _ in arrays),
        scratch_shapes=[pltpu.SemaphoreType.DMA((len(arrays),))],
        compiler_params=pltpu.CompilerParams(vmem_limit_bytes=4 * 2 ** 20),
        name="finish",
    )(*arrays)


def solution(mesh):
    groups = mesh.shape['model']

    def local_step(tokens, lengths, k_cache, v_cache, norm_gain, w_query, w_key, w_value, w_out, w_gate, w_up, w_down):
        kv_heads, _, head_dim = k_cache.shape[1:]
        packed = front(tokens, lengths, k_cache, v_cache, norm_gain, w_query, w_key, w_value, w_gate, w_up, groups)
        return back(packed, w_down, w_out, kv_heads, head_dim, groups)

    in_specs = (P('replica', None), P('replica'), P('replica', None, None, None), P('replica', None, None, None), P(None), P(None, 'model'), P(None, None), P(None, None), P('model', None), P(None, 'model'), P(None, 'model'), P('model', None))
    out_specs = (P('replica', None), P(('replica', 'model'), None, None), P(('replica', 'model'), None, None))
    return jax.shard_map(local_step, mesh=mesh, in_specs=in_specs, out_specs=out_specs, check_vma=False)
```

```python
import functools
import math

import jax
import jax.numpy as jnp
import numpy as np
from jax import lax
from jax.experimental import pallas as pl
from jax.experimental.pallas import tpu as pltpu
from jax.sharding import PartitionSpec as P

ROPE_BASE = 10000.0
NORM_EPS = 1e-6
MASK_VALUE = -1e30
MESH = pl.DeviceIdType.MESH
F32 = jnp.float32
BF16 = jnp.bfloat16
TILE = 256
SLOTS = 8
LEAD_NOW = 2
PIECES_NOW = 1
LAGS = (1, 6, 11, 13)
CHUNK = 64
UNROLL = 16
VMEM_BYTES = 67_043_328
RESULT_BYTES = 12_000_000
PIECES_SCORE = 13
PIECES_VALUE = 11
RING = 128


def front_kernel(lengths, tokens, gain_hbm, freq_hbm, k_cache, v_cache, w_query, w_key, w_value, w_gate, w_up,
                 packed,
                 x_buf, h_buf, w_buf, k_first, v_first, k_more, v_more, q_buf, kn_buf, vn_buf, fresh, score, peak, total, mixed, angle, rot,
                 gain, freq, o_out, kv_out, u_out,
                 item_seq, item_pos, out_sem, x_sem, w_sem, kf_sem, vf_sem, km_sem, vm_sem):
    batch, model_dim = tokens.shape
    head_dim = freq.shape[1]
    local_kv = kv_out.shape[1] // (2 * head_dim)
    heads = o_out.shape[1] // head_dim
    ratio = heads // local_kv
    q_tiles = w_query.shape[1] // TILE
    lead = q_tiles + 2
    half = TILE // 2
    pieces = w_gate.shape[1] // half
    ring_steps = RING // UNROLL
    first_steps = batch // UNROLL
    scale = head_dim ** -0.5
    me = lax.axis_index('model')
    local = pl.ds(me * local_kv, local_kv)
    lanes = local_kv * CHUNK

    def w_copy(src, tile, t):
        return pltpu.make_async_copy(src.at[:, pl.ds(pl.multiple_of(tile * TILE, TILE), TILE)], w_buf.at[t], w_sem.at[t])

    def start_piece(p, slot):
        for n, src in enumerate((w_gate, w_up)):
            pltpu.make_async_copy(src.at[:, pl.ds(pl.multiple_of(p * half, half), half)],
                                  w_buf.at[slot, :, n * half:(n + 1) * half], w_sem.at[slot]).start()

    def first_copy(cache, first, sem, step):
        rows = pl.ds(step * UNROLL, UNROLL)
        return pltpu.make_async_copy(cache.at[rows, local, pl.ds(0, CHUNK)], first.at[rows], sem.at[step])

    def start_items(cache, more, sem, step):
        at = lax.rem(step, ring_steps)
        for u in range(UNROLL):
            k = step * UNROLL + u
            pltpu.make_async_copy(cache.at[lax.rem(item_seq[k], batch), local, pl.ds(pl.multiple_of(item_pos[k], CHUNK), CHUNK)],
                                  more.at[at * UNROLL + u], sem.at[at]).start()

    x_copy = pltpu.make_async_copy(tokens, x_buf, x_sem.at[0])
    gain_copy = pltpu.make_async_copy(gain_hbm, gain, x_sem.at[1])
    freq_copy = pltpu.make_async_copy(freq_hbm, freq, x_sem.at[2])
    for copy in (freq_copy, x_copy, gain_copy):
        copy.start()
    lead_copies = [w_copy(w_key, me, 0), w_copy(w_value, me, 1)] + [w_copy(w_query, t, 2 + t) for t in range(q_tiles)]
    for copy in lead_copies[:LEAD_NOW]:
        copy.start()

    def second(i, k):
        for r in range(UNROLL):
            seq = i * UNROLL + r
            item_seq[k] = seq
            item_pos[k] = CHUNK
            k = k + (lengths[seq] > CHUNK).astype(jnp.int32)
        return k

    begin, end = 0, lax.fori_loop(0, batch // UNROLL, second, 0)
    for c in range(2, k_cache.shape[2] // CHUNK):
        def further(i, k):
            for r in range(4):
                at = begin + i * 4 + r
                seq = lax.rem(jnp.maximum(item_seq[at], 0), batch)
                item_seq[k] = seq
                item_pos[k] = c * CHUNK
                k = k + ((lengths[seq] > c * CHUNK) & (at < end)).astype(jnp.int32)
            return k

        begin, end = end, lax.fori_loop(0, lax.div(end - begin + 3, 4), further, end)
    steps = lax.div(end + (UNROLL - 1), UNROLL)

    for u in range(UNROLL):
        item_seq[end + u] = batch
        item_pos[end + u] = 0

    for copy in lead_copies[LEAD_NOW:]:
        copy.start()
    for step in range(first_steps):
        first_copy(k_cache, k_first, kf_sem, step).start()
    freq_copy.wait()

    @pl.loop(0, batch // 8)
    def _(i):
        for r in range(8):
            angle[pl.ds(i * 8 + r, 1), :] = lengths[i * 8 + r].astype(F32) * freq[...]

    first = lax.broadcasted_iota(jnp.int32, (batch, head_dim), 1) < head_dim // 2
    rot[0] = jnp.cos(angle[...])
    rot[1] = jnp.where(first, -jnp.sin(angle[...]), jnp.sin(angle[...]))
    q_buf[...] = jnp.zeros(q_buf.shape, F32)

    x_copy.wait()
    gain_copy.wait()
    for p in range(PIECES_NOW):
        start_piece(p, lead + p)
    x = x_buf[...].astype(F32)
    mean_sq = jnp.mean(x * x, axis=-1, keepdims=True)
    h_buf[...] = (x * lax.rsqrt(mean_sq + NORM_EPS) * gain[...].reshape(1, model_dim).astype(F32)).astype(BF16)

    def rope(a):
        return a * rot[0] + pltpu.roll(a, head_dim // 2, 1) * rot[1]

    for t, copy in enumerate(lead_copies):
        copy.wait()
        prod = jnp.dot(h_buf[...], w_buf[t], preferred_element_type=F32)
        if t == 0:
            for p in range(PIECES_NOW, SLOTS - lead):
                start_piece(p, lead + p)
        if t == 4:
            for step in range(first_steps):
                first_copy(v_cache, v_first, vf_sem, step).start()
        start_piece(SLOTS - lead + t, t)
        for j in range(TILE // head_dim):
            a = prod[:, j * head_dim:(j + 1) * head_dim]
            if t >= 2:
                q_buf[:, (t - 2) * (TILE // head_dim) + j, :] = rope(a).astype(BF16).astype(F32)
            else:
                a = (rope(a) if t == 0 else a).astype(BF16)
                col = (t * local_kv + j) * head_dim
                kv_out[:, col:col + head_dim] = a
                (kn_buf, vn_buf)[t][j] = a
    width = u_out.shape[1]
    o_at, kv_at = width, width + heads * head_dim
    x_at = kv_at + kv_out.shape[1]
    kv_copy = pltpu.make_async_copy(kv_out, packed.at[:, kv_at:x_at], out_sem.at[0])
    kv_copy.start()
    quarter = batch // 4
    x_part = model_dim // 4
    x_rows = pl.ds(pl.multiple_of(me * quarter, quarter), quarter)
    x_copies = [pltpu.make_async_copy(x_buf.at[x_rows, n * x_part:(n + 1) * x_part],
                                      packed.at[n * quarter:(n + 1) * quarter, x_at:x_at + x_part], out_sem.at[3 + n]) for n in range(4)]
    for copy in x_copies:
        copy.start()
    peak[batch] = jnp.full(peak.shape[1:], MASK_VALUE, F32)
    total[batch] = jnp.zeros(total.shape[1:], F32)
    mixed[batch] = jnp.zeros(mixed.shape[1:], F32)

    sub = q_buf.shape[1]
    lane = lax.broadcasted_iota(jnp.int32, (sub, lanes), 1)
    head = lax.broadcasted_iota(jnp.int32, (sub, lanes), 0)
    own = (lax.div(lane, CHUNK) == lax.div(head, ratio)) & (head < heads)
    pos_in = jnp.where(own, lax.rem(lane, CHUNK), 1 << 20)

    line = lax.broadcasted_iota(jnp.int32, (CHUNK, sub, lanes), 0)
    mine = line == pos_in[None]
    blocks = [slice(b0, b0 + CHUNK) for b0 in range(0, batch, CHUNK)]
    for rows in blocks:
        q = q_buf[rows].reshape(CHUNK * sub, head_dim).astype(BF16)
        s = lax.dot_general(q, kn_buf[:, rows].reshape(lanes, head_dim), (((1,), (1,)), ((), ())), preferred_element_type=F32) * scale
        s = jnp.where(mine, s.reshape(CHUNK, sub, lanes), MASK_VALUE)
        fresh[rows] = s
        peak[rows] = s

    def wait_first(first, sem, step):
        pltpu.make_async_copy(first.at[pl.ds(0, UNROLL)], first.at[pl.ds(step * UNROLL, UNROLL)], sem.at[step]).wait()

    def wait_more(more, sem, step):
        at = lax.rem(step, ring_steps)
        pltpu.make_async_copy(more.at[pl.ds(0, UNROLL)], more.at[pl.ds(at * UNROLL, UNROLL)], sem.at[at]).wait()

    def refill(cache, more, sem, step):
        @pl.when(step + ring_steps < steps)
        def _():
            start_items(cache, more, sem, step + ring_steps)

    def item(step, u, listed):
        k = step * UNROLL + u
        if listed:
            return batch + k, lax.rem(step, ring_steps) * UNROLL + u, item_seq[k], lax.rem(item_seq[k], batch), item_pos[k]
        return k, k, k, k, 0

    def score_step(step, listed):
        ring = k_more if listed else k_first
        found = []
        for u in range(UNROLL):
            k, at, seq, row, pos = item(step, u, listed)
            keys = ring[at].reshape(lanes, head_dim)
            s = lax.dot_general(q_buf[row].astype(BF16), keys, (((1,), (1,)), ((), ())), preferred_element_type=F32) * scale
            s = jnp.where(pos_in < lengths[row] - pos, s, MASK_VALUE)
            score[k] = s
            found.append((seq, s))
        for seq, s in found:
            peak[seq] = jnp.maximum(peak[seq], s)

    def value_step(step, listed):
        ring = v_more if listed else v_first
        found = []
        for u in range(UNROLL):
            k, at, seq, row, pos = item(step, u, listed)
            p = jnp.exp(score[k] - peak[seq])
            values = ring[at].reshape(lanes, head_dim)
            found.append((seq, p, jnp.dot(p.astype(BF16), values, preferred_element_type=F32)))
        for seq, p, o in found:
            total[seq] = total[seq] + p
            mixed[seq] = mixed[seq] + o

    def u_copy(p):
        cols = pl.ds(pl.multiple_of(p * half, half), half)
        return pltpu.make_async_copy(u_out.at[:, cols], packed.at[:, cols], out_sem.at[1])

    def wait_piece(p):
        slot = lax.rem(lead + p, SLOTS)
        pltpu.make_async_copy(w_gate.at[:, pl.ds(0, TILE)], w_buf.at[slot], w_sem.at[slot]).wait()

    def piece(p):
        prod = jnp.dot(h_buf[...], w_buf[lax.rem(lead + p, SLOTS)], preferred_element_type=F32)
        u_out[:, pl.ds(pl.multiple_of(p * half, half), half)] = (jax.nn.silu(prod[:, :half]) * prod[:, half:]).astype(BF16)

    def after_piece(p):
        u_copy(p).start()

        @pl.when(p + SLOTS < pieces)
        def _():
            start_piece(p + SLOTS, lax.rem(lead + p, SLOTS))

    def both(attend_step, cache, first, first_sem, more, more_sem, p0, p1):
        fetching = jnp.minimum(steps, first_steps)
        fused = jnp.minimum(steps, p1 - p0 - first_steps)

        def first_step(s, fetch):
            wait_first(first, first_sem, s)
            wait_piece(p0 + s)
            if fetch:
                start_items(cache, more, more_sem, s)
            attend_step(s, False)
            piece(p0 + s)
            after_piece(p0 + s)

        @pl.loop(0, fetching)
        def _(s):
            first_step(s, True)

        @pl.loop(fetching, first_steps)
        def _(s):
            first_step(s, False)

        @pl.loop(0, fused)
        def _(s):
            wait_more(more, more_sem, s)
            wait_piece(p0 + first_steps + s)
            attend_step(s, True)
            piece(p0 + first_steps + s)
            refill(cache, more, more_sem, s)
            after_piece(p0 + first_steps + s)

        @pl.loop(fused, steps)
        def _(s):
            wait_more(more, more_sem, s)
            attend_step(s, True)
            refill(cache, more, more_sem, s)

        return p0 + first_steps + fused

    reached = both(score_step, k_cache, k_first, kf_sem, k_more, km_sem, 0, PIECES_SCORE)

    @pl.loop(reached, PIECES_SCORE)
    def _(p):
        wait_piece(p)
        piece(p)
        after_piece(p)

    for rows in blocks:
        top = jnp.broadcast_to(jnp.max(peak[rows], axis=-1, keepdims=True), (CHUNK, sub, lanes))
        peak[rows] = top
        p = jnp.exp(fresh[rows] - top)
        total[rows] = p
        o = jnp.dot(p.reshape(CHUNK * sub, lanes).astype(BF16), vn_buf[:, rows].reshape(lanes, head_dim), preferred_element_type=F32)
        mixed[rows] = o.reshape(CHUNK, sub, head_dim)

    reached = both(value_step, v_cache, v_first, vf_sem, v_more, vm_sem, PIECES_SCORE, PIECES_SCORE + PIECES_VALUE)

    q_buf[...] = mixed[:batch] / jnp.sum(total[:batch], axis=-1, keepdims=True)
    for h in range(heads):
        o_out[:, h * head_dim:(h + 1) * head_dim] = q_buf[:, h, :].astype(BF16)
    o_copy = pltpu.make_async_copy(o_out, packed.at[:, o_at:kv_at], out_sem.at[2])
    o_copy.start()

    @pl.loop(reached, pieces)
    def _(p):
        wait_piece(p)
        piece(p)
        after_piece(p)

    kv_copy.wait()
    o_copy.wait()
    for copy in x_copies:
        copy.wait()
    pltpu.make_async_copy(u_out, packed.at[:, :width], out_sem.at[1]).wait()


def front(tokens, lengths, k_cache, v_cache, norm_gain, w_query, w_key, w_value, w_gate, w_up, groups):
    batch, model_dim = tokens.shape
    kv_heads, context, head_dim = k_cache.shape[1:]
    local_kv = kv_heads // groups
    q_dim = w_query.shape[1]
    width = w_gate.shape[1]
    half_freq = np.exp(np.arange(head_dim // 2) * (-2.0 * math.log(ROPE_BASE) / head_dim))
    freq = jnp.asarray(np.concatenate([half_freq, half_freq])[None, :], F32)
    items = batch * (context // CHUNK) + 2 * UNROLL
    lanes = local_kv * CHUNK
    dma = pltpu.SemaphoreType.DMA
    hbm = pl.BlockSpec(memory_space=pltpu.HBM)
    smem = pl.BlockSpec(memory_space=pltpu.SMEM)
    return pl.pallas_call(
        front_kernel,
        out_shape=jax.ShapeDtypeStruct((batch, width + q_dim + 2 * local_kv * head_dim + model_dim // 4), BF16),
        in_specs=[smem] + [hbm] * 10,
        out_specs=hbm,
        scratch_shapes=[
            pltpu.VMEM((batch, model_dim), BF16),
            pltpu.VMEM((batch, model_dim), BF16),
            pltpu.VMEM((SLOTS, model_dim, TILE), BF16),
            pltpu.VMEM((batch, local_kv, CHUNK, head_dim), BF16),
            pltpu.VMEM((batch, local_kv, CHUNK, head_dim), BF16),
            pltpu.VMEM((RING, local_kv, CHUNK, head_dim), BF16),
            pltpu.VMEM((RING, local_kv, CHUNK, head_dim), BF16),
            pltpu.VMEM((batch, 8, head_dim), F32),
            pltpu.VMEM((local_kv, batch, head_dim), BF16),
            pltpu.VMEM((local_kv, batch, head_dim), BF16),
            pltpu.VMEM((batch, 8, lanes), F32),
            pltpu.VMEM((items, 8, lanes), F32),
            pltpu.VMEM((batch + 1, 8, lanes), F32),
            pltpu.VMEM((batch + 1, 8, lanes), F32),
            pltpu.VMEM((batch + 1, 8, head_dim), F32),
            pltpu.VMEM((batch, head_dim), F32),
            pltpu.VMEM((2, batch, head_dim), F32),
            pltpu.VMEM((model_dim,), BF16),
            pltpu.VMEM((1, head_dim), F32),
            pltpu.VMEM((batch, q_dim), BF16),
            pltpu.VMEM((batch, 2 * local_kv * head_dim), BF16),
            pltpu.VMEM((batch, width), BF16),
            pltpu.SMEM((items,), jnp.int32),
            pltpu.SMEM((items,), jnp.int32),
            dma((7,)), dma((3,)), dma((SLOTS,)), dma((batch // UNROLL,)), dma((batch // UNROLL,)),
            dma((RING // UNROLL,)), dma((RING // UNROLL,)),
        ],
        compiler_params=pltpu.CompilerParams(vmem_limit_bytes=VMEM_BYTES),
        name="front",
    )(lengths, tokens, norm_gain, freq, k_cache, v_cache, w_query, w_key, w_value, w_gate, w_up)


def back_kernel(packed, w_down, w_out,
                y_out, key_out, value_out, _,
                u_buf, o_buf, kv_buf, x_buf, w_buf, wo_buf, part, from_sib, to_cross, from_cross, y_buf, kv_in, head_buf,
                in_sem, w_sem, wo_sem, kv_send, kv_recv, s1_send, s1_recv, s2_send, s2_recv,
                yc_send, yc_recv, ys_send, ys_recv, yr_send, yr_recv):
    me = lax.axis_index('model')
    core = lax.rem(me, 2)
    chip = lax.div(me, 2)
    sib = chip * 2 + (1 - core)
    cross = (1 - chip) * 2 + core
    diag = (1 - chip) * 2 + (1 - core)
    n_out = w_down.shape[1] // TILE
    head_dim = head_buf.shape[2]
    local_kv = kv_buf.shape[2] // (2 * head_dim)
    lag_sib, lag_cross, lag_relay, lag_store = LAGS

    barrier = pltpu.get_barrier_semaphore()
    for peer in (sib, cross, diag):
        pl.semaphore_signal(barrier, inc=1, device_id={'model': peer}, device_id_type=MESH)

    def cols(tile):
        return pl.ds(pl.multiple_of(tile * TILE, TILE), TILE)

    def down_copy(c):
        return pltpu.make_async_copy(w_down.at[:, cols(c)], w_buf.at[c], w_sem.at[c])

    def remote(src, dst, send, recv, peer):
        return pltpu.make_async_remote_copy(src_ref=src, dst_ref=dst, send_sem=send, recv_sem=recv,
                                            device_id={'model': peer}, device_id_type=MESH)

    def out_copy(c):
        return pltpu.make_async_copy(w_out.at[:, cols(c)], wo_buf.at[c], wo_sem.at[c])

    devices, rows = kv_buf.shape[:2]
    width, q_dim = u_buf.shape[1], o_buf.shape[1]
    kv_at = width + q_dim
    x_at = kv_at + kv_buf.shape[2]
    x_part = x_buf.shape[2]
    o_copy = pltpu.make_async_copy(packed.at[:, width:kv_at], o_buf, in_sem.at[0])
    u_copy = pltpu.make_async_copy(packed.at[:, :width], u_buf, in_sem.at[1])
    kv_copies = [pltpu.make_async_copy(packed.at[n * rows:(n + 1) * rows, kv_at:x_at], kv_buf.at[n], in_sem.at[2 + n]) for n in range(devices)]
    x_copies = [pltpu.make_async_copy(packed.at[n * rows:(n + 1) * rows, x_at:x_at + x_part], x_buf.at[n], in_sem.at[2 + devices + n])
                for n in range(devices)]
    for copy in (o_copy, u_copy, out_copy(0), down_copy(0), *kv_copies, *x_copies):
        copy.start()

    @pl.loop(1, n_out)
    def _(c):
        out_copy(c).start()
        down_copy(c).start()

    for copy in (o_copy, u_copy):
        copy.wait()

    kv_peers = (sib, cross, diag)

    def kv_copy(n):
        return remote(kv_buf.at[kv_peers[n]], kv_in.at[me], kv_send.at[n], kv_recv.at[n], kv_peers[n])

    def sib_send(c):
        return remote(part.at[c, :, 1 - core], from_sib.at[c], s1_send, s1_recv.at[c], sib)

    def cross_send(c):
        return remote(to_cross.at[c], from_cross.at[c], s2_send, s2_recv.at[c], cross)

    def y_cross(c):
        return remote(y_buf.at[c, me], y_buf.at[c, me], yc_send, yc_recv.at[c], cross)

    def y_sib(c):
        return remote(y_buf.at[c, me], y_buf.at[c, me], ys_send, ys_recv.at[c], sib)

    def y_relay(c):
        return remote(y_buf.at[c, cross], y_buf.at[c, cross], yr_send, yr_recv.at[c], sib)

    def product(c):
        out_copy(c).wait()
        total = jnp.dot(o_buf[...], wo_buf[c], preferred_element_type=F32)
        down_copy(c).wait()
        total += jnp.dot(u_buf[...], w_buf[c], preferred_element_type=F32)
        part[c] = total.reshape(part.shape[1:])

    for copy in kv_copies:
        copy.wait()
    pl.semaphore_wait(barrier, 3)
    for n in range(3):
        kv_copy(n).start()
    product(0)
    sib_send(0).start()
    for copy in x_copies:
        copy.wait()

    @pl.loop(1, n_out + lag_store)
    def _(i):
        @pl.when(i < n_out)
        def _():
            product(i)
            sib_send(i).start()

        @pl.when((i >= lag_sib) & (i < n_out + lag_sib))
        def _():
            c = i - lag_sib
            sib_send(c).wait_recv()
            to_cross[c] = part[c, 1 - chip, core] + from_sib[c, 1 - chip]
            cross_send(c).start()

        @pl.when((i >= lag_cross) & (i < n_out + lag_cross))
        def _():
            c = i - lag_cross
            cross_send(c).wait_recv()
            total = part[c, chip, core] + from_sib[c, chip] + from_cross[c]
            x = x_buf[lax.div(c * TILE, x_part), :, pl.ds(pl.multiple_of(lax.rem(c * TILE, x_part), TILE), TILE)]
            y_buf[c, me] = (x.astype(F32) + total).astype(BF16)
            y_cross(c).start()
            y_sib(c).start()

        @pl.when((i >= lag_relay) & (i < n_out + lag_relay))
        def _():
            c = i - lag_relay
            y_cross(c).wait_recv()
            y_relay(c).start()

        @pl.when(i == n_out)
        def _():
            for n in range(3):
                kv_copy(n).wait_recv()
            kv_in[me] = kv_buf[me]
            for half, out in enumerate((key_out, value_out)):
                for source in range(kv_in.shape[0]):
                    for g in range(local_kv):
                        start = (half * local_kv + g) * head_dim
                        head_buf[:, source * local_kv + g, :] = kv_in[source, :, start:start + head_dim].astype(F32)
                out[...] = head_buf[...].astype(BF16)

        @pl.when(i >= lag_store)
        def _():
            c = i - lag_store
            y_sib(c).wait_recv()
            y_relay(c).wait_recv()
            y_out[:, :, cols(c)] = y_buf[c]

    for n in range(3):
        kv_copy(n).wait_send()
    remote(part.at[:, :, 0], from_sib, s1_send, s1_recv.at[0], sib).wait_send()
    remote(to_cross, from_cross, s2_send, s2_recv.at[0], cross).wait_send()
    for sem in (yc_send, ys_send, yr_send):
        remote(y_buf.at[:, 0], y_buf.at[:, 0], sem, yc_recv.at[0], sib).wait_send()


def back(packed, w_down, w_out, kv_heads, head_dim, devices):
    batch = packed.shape[0]
    width, model_dim = w_down.shape
    q_dim = w_out.shape[0]
    rows = batch // devices
    n_out = model_dim // TILE
    kv_width = 2 * (kv_heads // devices) * head_dim
    dma = pltpu.SemaphoreType.DMA
    hbm = pl.BlockSpec(memory_space=pltpu.HBM)
    vmem = pl.BlockSpec(memory_space=pltpu.VMEM)
    y, key_out, value_out, _ = pl.pallas_call(
        back_kernel,
        out_shape=(jax.ShapeDtypeStruct((devices, rows, model_dim), BF16),
                   jax.ShapeDtypeStruct((rows, kv_heads, head_dim), BF16),
                   jax.ShapeDtypeStruct((rows, kv_heads, head_dim), BF16),
                   jax.ShapeDtypeStruct(packed.shape, BF16)),
        in_specs=[hbm] * 3,
        out_specs=(vmem, vmem, vmem, hbm),
        input_output_aliases={0: 3},
        scratch_shapes=[
            pltpu.VMEM((batch, width), BF16),
            pltpu.VMEM((batch, q_dim), BF16),
            pltpu.VMEM((devices, rows, kv_width), BF16),
            pltpu.VMEM((4, rows, model_dim // 4), BF16),
            pltpu.VMEM((n_out, width, TILE), BF16),
            pltpu.VMEM((n_out, q_dim, TILE), BF16),
            pltpu.VMEM((n_out, 2, 2, rows, TILE), F32),
            pltpu.VMEM((n_out, 2, rows, TILE), F32),
            pltpu.VMEM((n_out, rows, TILE), F32),
            pltpu.VMEM((n_out, rows, TILE), F32),
            pltpu.VMEM((n_out, devices, rows, TILE), BF16),
            pltpu.VMEM((devices, rows, kv_width), BF16),
            pltpu.VMEM((rows, kv_heads, head_dim), F32),
            dma((2 + 2 * devices,)), dma((n_out,)), dma((n_out,)), dma((3,)), dma((3,)),
        ] + [dma, dma((n_out,))] * 5,
        compiler_params=pltpu.CompilerParams(collective_id=0, has_side_effects=True, vmem_limit_bytes=VMEM_BYTES - RESULT_BYTES),
        name="back",
    )(packed, w_down, w_out)
    return finish(y.reshape(batch, model_dim), key_out, value_out)


def finish_kernel(*refs):
    half = (len(refs) - 1) // 2
    copies = [pltpu.make_async_copy(refs[n], refs[half + n], refs[-1].at[n]) for n in range(half)]
    for copy in copies:
        copy.start()
    for copy in copies:
        copy.wait()


def finish(*arrays):
    return pl.pallas_call(
        finish_kernel,
        out_shape=tuple(jax.ShapeDtypeStruct(a.shape, a.dtype) for a in arrays),
        in_specs=[pl.BlockSpec(memory_space=pltpu.VMEM)] * len(arrays),
        out_specs=tuple(pl.BlockSpec(memory_space=pltpu.HBM) for _ in arrays),
        scratch_shapes=[pltpu.SemaphoreType.DMA((len(arrays),))],
        compiler_params=pltpu.CompilerParams(vmem_limit_bytes=4 * 2 ** 20),
        name="finish",
    )(*arrays)


def solution(mesh):
    groups = mesh.shape['model']

    def local_step(tokens, lengths, k_cache, v_cache, norm_gain, w_query, w_key, w_value, w_out, w_gate, w_up, w_down):
        kv_heads, _, head_dim = k_cache.shape[1:]
        packed = front(tokens, lengths, k_cache, v_cache, norm_gain, w_query, w_key, w_value, w_gate, w_up, groups)
        return back(packed, w_down, w_out, kv_heads, head_dim, groups)

    in_specs = (P('replica', None), P('replica'), P('replica', None, None, None), P('replica', None, None, None), P(None), P(None, 'model'), P(None, None), P(None, None), P('model', None), P(None, 'model'), P(None, 'model'), P('model', None))
    out_specs = (P('replica', None), P(('replica', 'model'), None, None), P(('replica', 'model'), None, None))
    return jax.shard_map(local_step, mesh=mesh, in_specs=in_specs, out_specs=out_specs, check_vma=False)
```
